32 devices in a mesh: dp: 1 (over z), tp: 32 (over y, x, core).
Axes of the slice: x: 4, y: 4, z: 1, core: 2. Of those that a mesh axis runs over, the one named last changes fastest.
The devices are a block of a 4x4x8 slice.
Arguments:
- x_in: bfloat16 [1, 2048, 2048], P('dp', 'tp')
- y_grad: bfloat16 [1, 2048, 2048], P('dp', 'tp')
- ln_par: float32 [2, 4, 2048], replicated
- bias_d: float32 [2, 2, 2048], replicated
- w_qkv: bfloat16 [2, 2048, 3, 32, 64], P(None, None, None, 'tp')
- w_out: bfloat16 [2, 32, 64, 2048], P(None, 'tp')
- w_up: bfloat16 [2, 2048, 8192], P(None, None, 'tp')
- b_up: float32 [2, 8192], P(None, 'tp')
- w_down: bfloat16 [2, 8192, 2048], P(None, 'tp')
Outputs:
- output 1: bfloat16 [1, 2048, 2048], P('dp', 'tp')
- output 2: bfloat16 [1, 2048, 2048], P('dp', 'tp')
- output 3: float32 [2, 4, 2048], P('dp')
- output 4: float32 [2, 2, 2048], P('dp')
- output 5: bfloat16 [2, 2048, 3, 32, 64], P('dp', None, None, 'tp')
- output 6: bfloat16 [2, 32, 64, 2048], P('dp', 'tp')
- output 7: bfloat16 [2, 2048, 8192], P('dp', None, 'tp')
- output 8: float32 [2, 8192], P('dp', 'tp')
- output 9: bfloat16 [2, 8192, 2048], P('dp', 'tp')
All inputs are finite; a program needn't handle non-finite values.
Results may differ from the reference program's by a relative error of at most 0.02.
Values are sent between devices in bfloat16 or wider.
A program may use at most 768 MiB of HBM per device.

```python
import math
import jax
import jax.numpy as jnp
from jax import lax

N_BATCH = 1
SEQ_LEN = 2048
D_MODEL = 2048
N_HEADS = 32
HEAD_DIM = 64
FF_DIM = 8192
N_LAYERS = 2


def layer_norm(row_vals, ln_gain, ln_shift):
    mean_val = jnp.mean(row_vals, axis=-1, keepdims=True)
    centered = row_vals - mean_val
    var_val = jnp.mean(centered * centered, axis=-1, keepdims=True)
    return centered * lax.rsqrt(var_val + 1e-5) * ln_gain + ln_shift


def setup_inputs(seed: int = 0, part: int = 0) -> dict:
    part_key = jax.random.fold_in(jax.random.key(seed), part)
    part_list = jax.random.split(part_key, 3)
    key_list = jax.random.split(jax.random.key(seed + 1), 7)
    act_shape = (N_BATCH, SEQ_LEN, D_MODEL)
    token_scale = jax.random.uniform(part_list[0], (N_BATCH, SEQ_LEN, 1), jnp.float32, 0.5, 1.5)
    x_in = (jax.random.normal(part_list[1], act_shape, jnp.float32) * token_scale).astype(jnp.bfloat16)
    y_grad = jax.random.normal(part_list[2], act_shape, jnp.float32).astype(jnp.bfloat16)
    ln_base = jnp.array([1.0, 0.0, 1.0, 0.0], jnp.float32)[None, :, None]
    ln_par = ln_base + 0.2 * jax.random.normal(key_list[0], (N_LAYERS, 4, D_MODEL), jnp.float32)
    bias_d = 0.2 * jax.random.normal(key_list[1], (N_LAYERS, 2, D_MODEL), jnp.float32)
    qk_gain = (math.log(SEQ_LEN) / 2.0) ** 0.25
    qkv_gain = jnp.array([qk_gain, qk_gain, 1.0], jnp.float32)[None, None, :, None, None] * D_MODEL ** -0.5
    w_qkv = (jax.random.normal(key_list[2], (N_LAYERS, D_MODEL, 3, N_HEADS, HEAD_DIM), jnp.float32) * qkv_gain).astype(jnp.bfloat16)
    out_gain = 0.3 * SEQ_LEN ** 0.25 * D_MODEL ** -0.5
    w_out = (jax.random.normal(key_list[3], (N_LAYERS, N_HEADS, HEAD_DIM, D_MODEL), jnp.float32) * out_gain).astype(jnp.bfloat16)
    w_up = (jax.random.normal(key_list[4], (N_LAYERS, D_MODEL, FF_DIM), jnp.float32) * D_MODEL ** -0.5).astype(jnp.bfloat16)
    b_up = 0.5 * jax.random.normal(key_list[5], (N_LAYERS, FF_DIM), jnp.float32)
    w_down = (jax.random.normal(key_list[6], (N_LAYERS, FF_DIM, D_MODEL), jnp.float32) * FF_DIM ** -0.5).astype(jnp.bfloat16)
    return dict(x_in=x_in, y_grad=y_grad, ln_par=ln_par, bias_d=bias_d, w_qkv=w_qkv, w_out=w_out, w_up=w_up, b_up=b_up, w_down=w_down)


def head_attention(qkv_head):
    q_head = qkv_head[:, 0].astype(jnp.float32)
    k_head = qkv_head[:, 1].astype(jnp.float32)
    v_head = qkv_head[:, 2].astype(jnp.float32)
    scores = jnp.dot(q_head, k_head.T) * (HEAD_DIM ** -0.5)
    positions = jnp.arange(SEQ_LEN)
    causal = positions[:, None] >= positions[None, :]
    scores = jnp.where(causal, scores, -1e30)
    prob_bf = jax.nn.softmax(scores, axis=-1).astype(jnp.bfloat16)
    return jnp.dot(prob_bf.astype(jnp.float32), v_head).astype(jnp.bfloat16)


def attention_all(qkv_vals):
    per_head = jnp.transpose(qkv_vals, (0, 3, 1, 2, 4)).reshape(N_BATCH * N_HEADS, SEQ_LEN, 3, HEAD_DIM)
    head_out = lax.map(jax.checkpoint(head_attention), per_head)
    return jnp.transpose(head_out.reshape(N_BATCH, N_HEADS, SEQ_LEN, HEAD_DIM), (0, 2, 1, 3))


def block_forward(residual, layer_w):
    ln_vals, bias_vals, w_qkv, w_out, w_up, b_up, w_down = layer_w
    h_one = layer_norm(residual, ln_vals[0], ln_vals[1]).astype(jnp.bfloat16)
    qkv_vals = jnp.einsum('bsd,dche->bsche', h_one.astype(jnp.float32), w_qkv.astype(jnp.float32)).astype(jnp.bfloat16)
    attn_vals = attention_all(qkv_vals)
    attn_out = jnp.einsum('bshe,hed->bsd', attn_vals.astype(jnp.float32), w_out.astype(jnp.float32))
    residual = residual + attn_out + bias_vals[0]
    h_two = layer_norm(residual, ln_vals[2], ln_vals[3]).astype(jnp.bfloat16)
    pre_act = jnp.einsum('bsd,df->bsf', h_two.astype(jnp.float32), w_up.astype(jnp.float32)) + b_up
    act_vals = jax.nn.gelu(pre_act, approximate=True).astype(jnp.bfloat16)
    mlp_out = jnp.einsum('bsf,fd->bsd', act_vals.astype(jnp.float32), w_down.astype(jnp.float32))
    return residual + mlp_out + bias_vals[1]


def reference(x_in, y_grad, ln_par, bias_d, w_qkv, w_out, w_up, b_up, w_down):
    weights = (ln_par, bias_d, w_qkv, w_out, w_up, b_up, w_down)

    def forward(x_vals, layer_stack):
        def scan_body(residual, layer_w):
            return block_forward(residual, layer_w), None
        final_res, _ = lax.scan(scan_body, x_vals.astype(jnp.float32), layer_stack)
        return final_res

    final_res, pullback = jax.vjp(forward, x_in, weights)
    x_ct, w_ct = pullback(y_grad.astype(jnp.float32))
    return (final_res.astype(jnp.bfloat16), x_ct, w_ct[0], w_ct[1], w_ct[2], w_ct[3], w_ct[4], w_ct[5], w_ct[6])
```

```python
import functools
import math

import jax
import jax.numpy as jnp
from jax import lax
from jax.experimental import pallas as pl
from jax.experimental.pallas import tpu as pltpu
from jax.sharding import PartitionSpec as P

MESH = pl.DeviceIdType.MESH
BF = jnp.bfloat16
F32 = jnp.float32
LN_EPS = 1e-5
OFFS = (0, -1, 1, 2)
RS_ORDER = (2, 1, -1, 0)
PAIR = (0, 1)
WAYS = (1, -1)
LATE = (2, 3)
NN = ((1,), (0,))
NT = ((1,), (1,))
TN = ((0,), (0,))
MIB = 1 << 20
COMM_VMEM = [size * MIB for size in (12, 26, 26, 26, 22, 8, 20, 26)]
Q_BLOCKS = 8
ROW_CHUNK = 64
BACK_CHUNK = 64
ROW_UNROLL = 4
BACK_UNROLL = 2
LOG2E = math.log2(math.e)


def matmul(lhs, rhs, dims):
    return lax.dot_general(lhs, rhs, (dims, ((), ())), preferred_element_type=F32)


class Net:
    def __init__(self, group_size):
        side = math.isqrt(group_size // 2)
        me = lax.axis_index('tp')
        self.side = side
        self.core = lax.rem(me, 2)
        self.col = lax.rem(me // 2, side)
        self.row = me // (2 * side)

    def shift(self, pos, off):
        return lax.rem(pos + (off + self.side), self.side)

    def block(self, half, first, second):
        if half == 0:
            return self.shift(self.row, second), self.shift(self.col, first)
        return self.shift(self.row, first), self.shift(self.col, second)

    def neighbour(self, half, axis, sgn):
        if (axis == 0) == (half == 0):
            row, col = self.row, self.shift(self.col, sgn)
        else:
            row, col = self.shift(self.row, sgn), self.col
        return {'tp': (row * self.side + col) * 2 + self.core}

    def partner(self):
        return {'tp': (self.row * self.side + self.col) * 2 + (1 - self.core)}

    def pair_copy(self, src, dst, send_sem, recv_sem, num):
        return pltpu.make_async_remote_copy(src_ref=src, dst_ref=dst, send_sem=send_sem.at[num], recv_sem=recv_sem.at[num],
                                            device_id=self.partner(), device_id_type=MESH)

    def pair_barrier(self):
        sem = pltpu.get_barrier_semaphore()
        pl.semaphore_signal(sem, inc=1, device_id=self.partner(), device_id_type=MESH)
        pl.semaphore_wait(sem, 1)

    def barrier(self):
        sem = pltpu.get_barrier_semaphore()
        for half in PAIR:
            for sgn in WAYS:
                pl.semaphore_signal(sem, inc=1, device_id=self.neighbour(half, 0, sgn), device_id_type=MESH)
        pl.semaphore_wait(sem, 4)


class Gather:
    def __init__(self, net, buf, send_sem, recv_sem):
        self.net, self.buf, self.send_sem, self.recv_sem = net, buf, send_sem, recv_sem
        self.rows = buf.shape[2]
        self.sent = []

    def ident(self, half, stage, first, kind):
        return half * 20 + (0 if stage == 0 else 4 + 4 * OFFS.index(first)) + kind

    def slot(self, half, first, second, kind):
        row, col = self.net.block(half, first, second)
        n_half = self.rows // 2
        start, size = half * n_half, n_half
        if kind >= 2:
            size = n_half // 2
            start += (kind - 2) * size
        return self.buf.at[row, col, pl.ds(start, size)]

    def copy(self, half, stage, first, kind, ref):
        ident = self.ident(half, stage, first, kind)
        sgn = 1 if kind % 2 == 0 else -1
        return pltpu.make_async_remote_copy(
            src_ref=ref, dst_ref=ref, send_sem=self.send_sem.at[ident], recv_sem=self.recv_sem.at[ident],
            device_id=self.net.neighbour(half, stage, sgn), device_id_type=MESH)

    def send(self, half, stage, first, kind):
        back = (0, 0, -1, 1)[kind]
        offs = (back, 0) if stage == 0 else (first, back)
        copy = self.copy(half, stage, first, kind, self.slot(half, offs[0], offs[1], kind))
        copy.start()
        self.sent.append(copy)

    def wait(self, half, stage, first, kind):
        back = (-1, 1, 2, 2)[kind]
        offs = (back, 0) if stage == 0 else (first, back)
        self.copy(half, stage, first, kind, self.slot(half, offs[0], offs[1], kind)).wait_recv()

    def each(self, call, stage, first, kinds):
        for kind in kinds:
            for half in PAIR:
                call(half, stage, first, kind)

    def onward(self, half, stage, first, kind):
        self.wait(half, stage, first, kind)
        self.send(half, stage, first, kind + 2)

    def run(self):
        self.each(self.send, 0, 0, PAIR)
        self.each(self.send, 1, 0, PAIR)
        for kind in PAIR:
            for half in PAIR:
                self.onward(half, 0, 0, kind)
                for way in PAIR:
                    self.send(half, 1, -WAYS[kind], way)
        self.each(self.onward, 1, 0, PAIR)
        self.each(self.wait, 0, 0, LATE)
        self.each(self.send, 1, 2, PAIR)
        for first in OFFS[1:]:
            self.each(self.onward, 1, first, PAIR)
        for first in OFFS:
            self.each(self.wait, 1, first, LATE)
        for copy in self.sent:
            copy.wait_send()


class Scatter:
    def __init__(self, net, part, recv, out, held, send_sem, recv_sem):
        self.net, self.part, self.recv, self.out, self.held = net, part, recv, out, held
        self.send_sem, self.recv_sem = send_sem, recv_sem
        self.quarter = part.shape[2] // 4
        self.sent = []

    def copy(self, half, stage, way, kind, ref):
        ident = ((half * 5 + stage) * 2 + way) * 3 + kind
        return pltpu.make_async_remote_copy(
            src_ref=ref, dst_ref=self.recv.at[half, stage, way, kind],
            send_sem=self.send_sem.at[ident], recv_sem=self.recv_sem.at[ident],
            device_id=self.net.neighbour(half, 0 if stage == 4 else 1, WAYS[way]), device_id_type=MESH)

    def send(self, half, stage, way, kind, ref):
        copy = self.copy(half, stage, way, kind, ref)
        copy.start()
        self.sent.append(copy)

    def wait(self, half, stage, way, kind):
        self.copy(half, stage, way, kind, self.recv.at[half, stage, way, kind]).wait_recv()

    def term(self, half, stage, off, sub):
        if stage == 4:
            return self.held.at[half, {2: 0, 1: 1, -1: 2}[off], pl.ds(sub * self.quarter, self.quarter)]
        row, col = self.net.block(half, RS_ORDER[stage], off)
        return self.part.at[row, col, pl.ds((2 * half + sub) * self.quarter, self.quarter)]

    def far(self, half, stage):
        for way in PAIR:
            self.send(half, stage, way, 0, self.term(half, stage, 2, way))

    def near_plain(self, half, stage, way):
        self.send(half, stage, way, 1, self.term(half, stage, WAYS[way], 1 - way))

    def near_summed(self, half, stage, way):
        self.wait(half, stage, way, 0)
        total = self.term(half, stage, WAYS[way], way)[...].astype(F32) + self.recv[half, stage, way, 0].astype(F32)
        self.out[half, stage, way] = total.astype(BF)
        self.send(half, stage, way, 2, self.out.at[half, stage, way])

    def arrived(self, half, stage, sub):
        first = self.recv[half, stage, 0, 2 if sub == 0 else 1].astype(F32)
        second = self.recv[half, stage, 1, 1 if sub == 0 else 2].astype(F32)
        return first + second

    def finish(self, half, stage):
        for way in PAIR:
            self.wait(half, stage, way, 1)
            self.wait(half, stage, way, 2)
        for sub in PAIR:
            total = self.term(half, stage, 0, sub)[...].astype(F32) + self.arrived(half, stage, sub)
            rows = pl.ds(sub * self.quarter, self.quarter)
            if stage < 3:
                self.held[half, stage, rows] = total.astype(BF)
            else:
                self.last[half, rows] = total

    def run(self, last):
        self.last = last
        for stage in range(4):
            for half in PAIR:
                self.far(half, stage)
        for stage in range(3):
            for half in PAIR:
                for way in PAIR:
                    self.near_summed(half, stage, way)
                    self.near_plain(half, stage, way)
        for half in PAIR:
            self.finish(half, 0)
            self.far(half, 4)
        for half in PAIR:
            for way in PAIR:
                self.near_summed(half, 3, way)
                self.near_plain(half, 3, way)
        for stage in (1, 2):
            for half in PAIR:
                self.finish(half, stage)
                self.near_plain(half, 4, stage - 1)
        for half in PAIR:
            for way in PAIR:
                self.near_summed(half, 4, way)
        for half in PAIR:
            self.finish(half, 3)
        for half in PAIR:
            for way in PAIR:
                self.wait(half, 4, way, 1)
                self.wait(half, 4, way, 2)
            for sub in PAIR:
                rows = pl.ds(sub * self.quarter, self.quarter)
                last[half, rows] = last[half, rows] + self.arrived(half, 4, sub)
        for copy in self.sent:
            copy.wait_send()


def gather_scratch():
    return [pltpu.SemaphoreType.DMA((40,)), pltpu.SemaphoreType.DMA((40,))]


def scatter_scratch(rows, width):
    quarter = rows // 4
    return [pltpu.VMEM((2, 5, 2, 3, quarter, width), BF),
            pltpu.VMEM((2, 5, 2, quarter, width), BF),
            pltpu.VMEM((2, 3, 2 * quarter, width), BF),
            pltpu.VMEM((2, 2 * quarter, width), F32),
            pltpu.SemaphoreType.DMA((60,)), pltpu.SemaphoreType.DMA((60,))]


def vmem_specs(count):
    return [pl.BlockSpec(memory_space=pltpu.VMEM)] * count


def comm_params(ident):
    return pltpu.CompilerParams(collective_id=ident, has_side_effects=True, vmem_limit_bytes=COMM_VMEM[ident])


def normalised(vals):
    mean_val = jnp.mean(vals, axis=-1, keepdims=True)
    centered = vals - mean_val
    var_val = jnp.mean(centered * centered, axis=-1, keepdims=True)
    inv_std = lax.rsqrt(var_val + LN_EPS)
    return centered * inv_std, inv_std


def norm_backward(d_out, vals, gain):
    unit, inv_std = normalised(vals)
    d_unit = d_out * gain
    mean_d = jnp.mean(d_unit, axis=-1, keepdims=True)
    mean_du = jnp.mean(d_unit * unit, axis=-1, keepdims=True)
    d_vals = inv_std * (d_unit - mean_d - unit * mean_du)
    return d_vals, jnp.sum(d_out * unit, axis=0, keepdims=True), jnp.sum(d_out, axis=0, keepdims=True)


def col_sum(vals):
    return jnp.sum(vals, axis=0, keepdims=True)


def first_kernel(group_size, x_ref, par_ref, h_ref, g_send, g_recv):
    net = Net(group_size)
    unit, _ = normalised(x_ref[...].astype(F32))
    h_ref[net.row, net.col] = (unit * par_ref[0:1] + par_ref[1:2]).astype(BF)
    net.barrier()
    Gather(net, h_ref, g_send, g_recv).run()


def forward_kernel(group_size, part_ref, res_ref, par_ref, new_ref, h_ref, recv, out, held, last, s_send, s_recv, g_send, g_recv):
    net = Net(group_size)
    rows, width = res_ref.shape
    net.barrier()
    Scatter(net, part_ref, recv, out, held, s_send, s_recv).run(last)
    new = res_ref[...] + last[...].reshape(rows, width) + par_ref[0:1]
    new_ref[...] = new
    unit, _ = normalised(new)
    h_ref[net.row, net.col] = (unit * par_ref[1:2] + par_ref[2:3]).astype(BF)
    Gather(net, h_ref, g_send, g_recv).run()


def turn_kernel(group_size, part_ref, res_ref, par_ref, dy_ref, y_ref, sum_ref, d_ref, recv, out, held, last, s_send, s_recv, g_send, g_recv):
    net = Net(group_size)
    rows, width = res_ref.shape
    d_ref[net.row, net.col] = dy_ref[...]
    net.barrier()
    Scatter(net, part_ref, recv, out, held, s_send, s_recv).run(last)
    y_ref[...] = (res_ref[...] + last[...].reshape(rows, width) + par_ref[0:1]).astype(BF)
    sum_ref[0:1] = col_sum(dy_ref[...].astype(F32))
    Gather(net, d_ref, g_send, g_recv).run()


def backward_kernel(group_size, part_ref, res_ref, par_ref, dres_ref, new_ref, sum_ref, d_ref, recv, out, held, last, s_send, s_recv, g_send, g_recv):
    net = Net(group_size)
    rows, width = res_ref.shape
    net.barrier()
    Scatter(net, part_ref, recv, out, held, s_send, s_recv).run(last)
    d_vals, d_gain, d_shift = norm_backward(last[...].reshape(rows, width), res_ref[...], par_ref[0:1])
    new = dres_ref[...] + d_vals
    new_ref[...] = new
    d_ref[net.row, net.col] = new.astype(BF)
    sum_ref[0:1] = d_gain
    sum_ref[1:2] = d_shift
    sum_ref[2:3] = col_sum(new)
    Gather(net, d_ref, g_send, g_recv).run()


def last_kernel(group_size, part_ref, res_ref, par_ref, dres_ref, new_ref, sum_ref, recv, out, held, last, s_send, s_recv):
    net = Net(group_size)
    rows, width = res_ref.shape
    net.barrier()
    Scatter(net, part_ref, recv, out, held, s_send, s_recv).run(last)
    d_vals, d_gain, d_shift = norm_backward(last[...].reshape(rows, width), res_ref[...], par_ref[0:1])
    new_ref[...] = (dres_ref[...] + d_vals).astype(BF)
    sum_ref[0:1] = d_gain
    sum_ref[1:2] = d_shift


def sum_kernel(group_size, in_ref, out_ref, buf, sem_s, sem_r):
    net = Net(group_size)
    sem = pltpu.get_barrier_semaphore()
    targets = [[(net.row, net.shift(net.col, off)) for off in (1, 2, 3)], [(net.shift(net.row, off), net.col) for off in (1, 2, 3)]]
    devs = [[{'tp': (row * net.side + col) * 2 + net.core} for row, col in pair] for pair in targets]
    for dev in devs[0] + devs[1] + [net.partner()]:
        pl.semaphore_signal(sem, inc=1, device_id=dev, device_id_type=MESH)
    pl.semaphore_wait(sem, 7)
    value = in_ref[...]
    for axis in PAIR:
        own = net.col if axis == 0 else net.row
        buf[axis, own] = value
        copies = []
        for num, dev in enumerate(devs[axis]):
            copies.append(pltpu.make_async_remote_copy(
                src_ref=buf.at[axis, own], dst_ref=buf.at[axis, own], send_sem=sem_s.at[axis * 3 + num],
                recv_sem=sem_r.at[axis * 3 + num], device_id=dev, device_id_type=MESH))
            copies[-1].start()
        for copy in copies:
            copy.wait_recv()
        value = buf[axis, 0] + buf[axis, 1] + buf[axis, 2] + buf[axis, 3]
        for copy in copies:
            copy.wait_send()
    buf[2, 0] = value
    copy = pltpu.make_async_remote_copy(src_ref=buf.at[2, 0], dst_ref=buf.at[2, 1], send_sem=sem_s.at[6], recv_sem=sem_r.at[6],
                                        device_id=net.partner(), device_id_type=MESH)
    copy.start()
    copy.wait()
    out_ref[...] = value + buf[2, 1]


def gelu_tanh(pre_act):
    return jax.nn.gelu(pre_act, approximate=True)


def attention_kernel(group_size, qkv_ref, nat_ref, stat_ref, a_ref, send, score, prob, a_nat, a_part, send_sem, recv_sem):
    net = Net(group_size)
    net.pair_barrier()
    parts, n_blk, _, rows, head = nat_ref.shape
    core, n_plane = net.core, n_blk * rows
    for part in range(parts):
        send[part] = qkv_ref[:, (parts + part) * head:(parts + part + 1) * head].reshape(n_blk, rows, head)
    copies = [net.pair_copy(send, nat_ref.at[:, :, core], send_sem, recv_sem, 0)]
    copies[0].start()
    for part in range(parts):
        nat_ref[part, :, core] = qkv_ref[:, part * head:(part + 1) * head].reshape(n_blk, rows, head)
    copies[0].wait_recv()
    step = n_blk // Q_BLOCKS
    n_q = 2 * step * rows
    factor = head ** -0.5 * LOG2E
    for blk in range(Q_BLOCKS):
        here, upto, left = pl.ds(blk * step, step), (blk + 1) * step, blk * n_q
        size = left + n_q
        score[:, :size] = matmul(nat_ref[0, here].reshape(n_q, head), nat_ref[1, :upto].reshape(size, head), NT)

        def softmax_rows(num, carry):
            row = pl.ds(pl.multiple_of(num * ROW_CHUNK, ROW_CHUNK), ROW_CHUNK)
            vals = [score[row, :left]] if left else []
            vals.append(masked(score[row, left:size], num * ROW_CHUNK))
            top = functools.reduce(jnp.maximum, [jnp.max(val, axis=1, keepdims=True) for val in vals])
            exps = [jnp.exp2((val - top) * factor) for val in vals]
            inv = 1.0 / sum(jnp.sum(val, axis=1, keepdims=True) for val in exps)
            if left:
                prob[row, :left] = (exps[0] * inv).astype(BF)
            prob[row, left:size] = (exps[-1] * inv).astype(BF)
            stat = pl.ds(pl.multiple_of(left + num * ROW_CHUNK, ROW_CHUNK), ROW_CHUNK)
            stat_ref[0, stat] = top
            stat_ref[1, stat] = inv
            return carry

        lax.fori_loop(0, n_q // ROW_CHUNK, softmax_rows, 0, unroll=ROW_UNROLL)
        attn = matmul(prob[:, :size], nat_ref[2, :upto].reshape(size, head), NN).astype(BF)
        a_nat[here] = attn.reshape(step, 2, rows, head)
        copies.append(net.pair_copy(a_nat.at[here, 1 - core], a_part.at[here], send_sem, recv_sem, 1 + blk))
        copies[-1].start()
    a_ref[:, :head] = a_nat[:, core].reshape(n_plane, head)
    for copy in copies[1:]:
        copy.wait_recv()
    a_ref[:, head:] = a_part[...].reshape(n_plane, head)
    for copy in copies:
        copy.wait_send()


def masked(vals, first_row):
    row = first_row + lax.broadcasted_iota(jnp.int32, vals.shape, 0)
    return jnp.where(row >= lax.broadcasted_iota(jnp.int32, vals.shape, 1), vals, -1e30)


def attention_back_kernel(group_size, d_ref, nat_ref, stat_ref, dq_ref, send, d_nat, score, d_prob, prob, d_score, dk_acc, dv_acc,
                          g_nat, g_part, send_sem, recv_sem):
    net = Net(group_size)
    net.pair_barrier()
    parts, n_blk, _, rows, head = nat_ref.shape
    core, n_plane = net.core, n_blk * rows
    send[...] = d_ref[:, head:].reshape(n_blk, rows, head)
    copies = [net.pair_copy(send, d_nat.at[:, core], send_sem, recv_sem, 0)]
    copies[0].start()
    d_nat[:, core] = d_ref[:, :head].reshape(n_blk, rows, head)
    copies[0].wait_recv()
    step = n_blk // Q_BLOCKS
    n_q = 2 * step * rows
    scale = head ** -0.5
    for blk in reversed(range(Q_BLOCKS)):
        here, upto, left = pl.ds(blk * step, step), (blk + 1) * step, blk * n_q
        size = left + n_q
        q_vals = nat_ref[0, here].reshape(n_q, head)
        k_vals = nat_ref[1, :upto].reshape(size, head)
        d_vals = d_nat[here].reshape(n_q, head)
        score[:, :size] = matmul(q_vals, k_vals, NT)
        d_prob[:, :size] = matmul(d_vals, nat_ref[2, :upto].reshape(size, head), NT)

        def score_rows(num, carry):
            row = pl.ds(pl.multiple_of(num * BACK_CHUNK, BACK_CHUNK), BACK_CHUNK)
            stat = pl.ds(pl.multiple_of(left + num * BACK_CHUNK, BACK_CHUNK), BACK_CHUNK)
            top, inv = stat_ref[0, stat], stat_ref[1, stat]
            cols = [slice(0, left)] if left else []
            cols.append(slice(left, size))
            probs = []
            for col in cols:
                val = score[row, col]
                if col is cols[-1]:
                    val = masked(val, num * BACK_CHUNK)
                probs.append((jnp.exp2((val - top) * (scale * LOG2E)) * inv).astype(BF))
                prob[row, col] = probs[-1]
            wide = [val.astype(F32) for val in probs]
            grads = [d_prob[row, col] for col in cols]
            dot = sum(jnp.sum(val * grad, axis=1, keepdims=True) for val, grad in zip(wide, grads))
            for col, val, grad in zip(cols, wide, grads):
                d_score[row, col] = (val * (grad - dot) * scale).astype(BF)
            return carry

        lax.fori_loop(0, n_q // BACK_CHUNK, score_rows, 0, unroll=BACK_UNROLL)
        g_nat[0, here] = matmul(d_score[:, :size], k_vals, NN).astype(BF).reshape(step, 2, rows, head)
        for acc, lhs, rhs in ((dk_acc, d_score, q_vals), (dv_acc, prob, d_vals)):
            term = matmul(lhs[:, :size], rhs, TN)
            if blk + 1 == Q_BLOCKS:
                acc[...] = term
            else:
                acc[:size] = acc[:size] + term
        for part, acc in ((1, dk_acc), (2, dv_acc)):
            g_nat[part, here] = acc[left:size].astype(BF).reshape(step, 2, rows, head)
        copies.append(net.pair_copy(g_nat.at[:, here, 1 - core], g_part.at[:, here], send_sem, recv_sem, 1 + blk))
        copies[-1].start()
    for part in range(parts):
        dq_ref[:, part * head:(part + 1) * head] = g_nat[part, :, core].reshape(n_plane, head)
    for copy in copies[1:]:
        copy.wait_recv()
    for part in range(parts):
        dq_ref[:, (parts + part) * head:(parts + part + 1) * head] = g_part[part].reshape(n_plane, head)
    for copy in copies:
        copy.wait_send()


def solution(mesh):
    group_size = mesh.shape['tp']
    side = math.isqrt(group_size // 2)
    if 2 * side * side != group_size or side != len(OFFS):
        raise ValueError('unsupported group')
    swap = [(dev, dev + 1 - 2 * (dev % 2)) for dev in range(group_size)]

    def device_step(x_loc, dy_loc, ln_par, bias_d, w_qkv, w_out, w_up, b_up, w_down):
        n_layers, width = ln_par.shape[0], x_loc.shape[-1]
        rows = x_loc.shape[1]
        n_plane = rows * side * side
        head = w_qkv.shape[-1]
        n_col = w_up.shape[-1]
        plane = jax.ShapeDtypeStruct((side, side, rows, width), BF)
        local_f = jax.ShapeDtypeStruct((rows, width), F32)
        local_b = jax.ShapeDtypeStruct((rows, width), BF)

        def sums(count):
            return jax.ShapeDtypeStruct((count, width), F32)

        def comm(kernel, ident, args, outs, scratch):
            return pl.pallas_call(
                functools.partial(kernel, group_size), name=kernel.__name__, out_shape=outs,
                in_specs=vmem_specs(len(args)), out_specs=jax.tree.map(lambda _: vmem_specs(1)[0], outs),
                scratch_shapes=scratch, compiler_params=comm_params(ident))(*args)

        block_shape = (side * side, rows, head)
        nat_shape = jax.ShapeDtypeStruct((3, side * side, 2, rows, head), BF)
        n_all, n_q = 2 * n_plane, 2 * n_plane // Q_BLOCKS
        stat_shape = jax.ShapeDtypeStruct((2, n_all, 1), F32)
        pair_sems = [pltpu.SemaphoreType.DMA((1 + Q_BLOCKS,))] * 2

        both_scratch = scatter_scratch(rows, width) + gather_scratch()

        def swapped(vals):
            return lax.ppermute(vals, 'tp', swap)

        def blocks(part):
            return part.astype(BF).reshape(side, side, rows, width)

        wq_mine = w_qkv.reshape(n_layers, width, 3 * head)
        wq_both = jnp.concatenate([wq_mine, swapped(wq_mine)], axis=2)
        wo_mine = w_out.reshape(n_layers, head, width)
        wo_both = jnp.concatenate([wo_mine, swapped(wo_mine)], axis=1)
        wu_both = jnp.concatenate([w_up, swapped(w_up)], axis=2)
        wd_both = jnp.concatenate([w_down, swapped(w_down)], axis=1)
        bu_both = jnp.concatenate([b_up, swapped(b_up)], axis=1)

        x_rows = x_loc.reshape(rows, width)
        dy_rows = dy_loc.reshape(rows, width)
        h_plane = comm(first_kernel, 0, [x_rows, ln_par[0, 0:2]], plane, gather_scratch())
        res_one = x_rows.astype(F32)
        saved = []
        for layer in range(n_layers):
            h_flat = h_plane.reshape(n_plane, width)
            qkv = matmul(h_flat, wq_both[layer], NN).astype(BF)
            nat, stat, a_both = comm(attention_kernel, 6, [qkv], (nat_shape, stat_shape, jax.ShapeDtypeStruct((n_plane, 2 * head), BF)), [
                pltpu.VMEM((3,) + block_shape, BF), pltpu.VMEM((n_q, n_all), F32), pltpu.VMEM((n_q, n_all), BF),
                pltpu.VMEM(nat_shape.shape[1:], BF), pltpu.VMEM(block_shape, BF)] + pair_sems)
            part = blocks(matmul(a_both, wo_both[layer], NN))
            par = jnp.concatenate([bias_d[layer, 0:1], ln_par[layer, 2:4]], axis=0)
            res_two, h2_plane = comm(forward_kernel, 1, [part, res_one, par], (local_f, plane), both_scratch)
            h2_flat = h2_plane.reshape(n_plane, width)
            pre_act = matmul(h2_flat, wu_both[layer], NN) + bu_both[layer]
            act_f, gelu_pull = jax.vjp(gelu_tanh, pre_act)
            act = act_f.astype(BF)
            part = blocks(matmul(act, wd_both[layer], NN))
            saved.append((res_one, h_flat, nat, stat, a_both, res_two, h2_flat, gelu_pull, act))
            if layer + 1 < n_layers:
                par = jnp.concatenate([bias_d[layer, 1:2], ln_par[layer + 1, 0:2]], axis=0)
                res_one, h_plane = comm(forward_kernel, 1, [part, res_two, par], (local_f, plane), both_scratch)
            else:
                y_rows, top_sum, d_plane = comm(turn_kernel, 2, [part, res_two, bias_d[layer, 1:2], dy_rows],
                                                (local_b, sums(1), plane), both_scratch)

        d_res = dy_rows.astype(F32)
        bias_two = top_sum[0:1]
        grads = [None] * n_layers
        for layer in reversed(range(n_layers)):
            res_one, h_flat, nat, stat, a_both, res_two, h2_flat, gelu_pull, act = saved[layer]
            d_flat = d_plane.reshape(n_plane, width)
            d_act = matmul(d_flat, wd_both[layer], NT)
            d_pre = gelu_pull(d_act)[0]
            d_pre_bf = d_pre.astype(BF)
            d_bup = jnp.sum(d_pre, axis=0)
            part = blocks(matmul(d_pre_bf, wu_both[layer], NT))
            d_res, sum_two, da_plane = comm(backward_kernel, 3, [part, res_two, ln_par[layer, 2:3], d_res],
                                            (local_f, sums(3), plane), both_scratch)
            d_wdown = matmul(act, d_flat, TN)
            d_wup = matmul(h2_flat, d_pre_bf, TN)
            da_flat = da_plane.reshape(n_plane, width)
            d_both = matmul(da_flat, wo_both[layer], NT).astype(BF)
            dq_both = comm(attention_back_kernel, 7, [d_both, nat, stat], jax.ShapeDtypeStruct((n_plane, 6 * head), BF), [
                pltpu.VMEM(block_shape, BF), pltpu.VMEM(nat_shape.shape[1:], BF), pltpu.VMEM((n_q, n_all), F32),
                pltpu.VMEM((n_q, n_all), F32), pltpu.VMEM((n_q, n_all), BF), pltpu.VMEM((n_q, n_all), BF),
                pltpu.VMEM((n_all, head), F32), pltpu.VMEM((n_all, head), F32), pltpu.VMEM(nat_shape.shape, BF),
                pltpu.VMEM((3,) + block_shape, BF)] + pair_sems)
            part = blocks(matmul(dq_both, wq_both[layer], NT))
            args = [part, res_one, ln_par[layer, 0:1], d_res]
            d_wout = matmul(a_both, da_flat, TN)
            d_wqkv = matmul(h_flat, dq_both, TN)
            if layer > 0:
                d_res, sum_one, d_plane = comm(backward_kernel, 3, args, (local_f, sums(3), plane), both_scratch)
                next_two = sum_one[2:3]
            else:
                x_grad, sum_one = comm(last_kernel, 4, args, (local_b, sums(2)), scatter_scratch(rows, width))
                next_two = None
            small = jnp.concatenate([sum_one[0:2], sum_two[0:2], sum_two[2:3], bias_two], axis=0)
            bias_two = next_two
            grads[layer] = (
                small,
                (d_wqkv[:, :3 * head] + swapped(d_wqkv[:, 3 * head:].astype(BF)).astype(F32)).astype(BF),
                (d_wout[:head] + swapped(d_wout[head:].astype(BF)).astype(F32)).astype(BF),
                (d_wup[:, :n_col] + swapped(d_wup[:, n_col:].astype(BF)).astype(F32)).astype(BF),
                d_bup[:n_col] + swapped(d_bup[n_col:]),
                (d_wdown[:n_col] + swapped(d_wdown[n_col:].astype(BF)).astype(F32)).astype(BF))
        n_small = grads[0][0].shape[0]
        packed = jnp.concatenate([grad[0] for grad in grads], axis=0)
        pad = -packed.shape[0] % 8
        packed = jnp.concatenate([packed, jnp.zeros((pad, width), F32)], axis=0)
        total = comm(sum_kernel, 5, [packed], sums(packed.shape[0]),
                     [pltpu.VMEM((3, side) + packed.shape, F32), pltpu.SemaphoreType.DMA((7,)), pltpu.SemaphoreType.DMA((7,))])
        total = total[:n_small * n_layers].reshape(n_layers, n_small, width)
        return (y_rows.reshape(x_loc.shape), x_grad.reshape(x_loc.shape), total[:, :4], total[:, 4:],
                jnp.stack([grad[1].reshape(width, 3, 1, head) for grad in grads]),
                jnp.stack([grad[2].reshape(1, head, width) for grad in grads]),
                jnp.stack([grad[3] for grad in grads]),
                jnp.stack([grad[4] for grad in grads]),
                jnp.stack([grad[5] for grad in grads]))

    def on_tp(dim, first=None):
        return P(first, *[None] * (dim - 1), 'tp')

    rows_spec = P('dp', 'tp')
    in_specs = (rows_spec, rows_spec, P(), P(), on_tp(3), on_tp(1), on_tp(2), on_tp(1), on_tp(1))
    out_specs = (rows_spec, rows_spec, P('dp'), P('dp'), on_tp(3, 'dp'), on_tp(1, 'dp'), on_tp(2, 'dp'), on_tp(1, 'dp'), on_tp(1, 'dp'))
    return jax.shard_map(device_step, mesh=mesh, in_specs=in_specs, out_specs=out_specs, check_vma=False)
```

```python
import functools
import math

import jax
import jax.numpy as jnp
from jax import lax
from jax.experimental import pallas as pl
from jax.experimental.pallas import tpu as pltpu
from jax.sharding import PartitionSpec as P

MESH = pl.DeviceIdType.MESH
BF = jnp.bfloat16
F32 = jnp.float32
LN_EPS = 1e-5
OFFS = (0, -1, 1, 2)
RS_ORDER = (2, 1, -1, 0)
PAIR = (0, 1)
WAYS = (1, -1)
LATE = (2, 3)
NN = ((1,), (0,))
NT = ((1,), (1,))
TN = ((0,), (0,))
MIB = 1 << 20
COMM_VMEM = [size * MIB for size in (4, 10, 6, 16, 14, 14, 12, 20, 20)]
Q_BLOCKS = 8
ROW_CHUNK = 64
BACK_CHUNK = 64
ROW_UNROLL = 4
BACK_UNROLL = 2
LOG2E = math.log2(math.e)
BOTH_ORDER = 'axaaaxaaaaaamccxccxcccc'
SCATTER_ORDER = 'axaxaaxaaxaaam'
WORK_CHUNK = 512
GATHER_PLAN = [1] * Q_BLOCKS


def matmul(lhs, rhs, dims):
    return lax.dot_general(lhs, rhs, (dims, ((), ())), preferred_element_type=F32)


class Net:
    def __init__(self, group_size):
        side = math.isqrt(group_size // 2)
        me = lax.axis_index('tp')
        self.side = side
        self.core = lax.rem(me, 2)
        self.col = lax.rem(me // 2, side)
        self.row = me // (2 * side)

    def shift(self, pos, off):
        return lax.rem(pos + (off + self.side), self.side)

    def block(self, half, first, second):
        if half == 0:
            return self.shift(self.row, second), self.shift(self.col, first)
        return self.shift(self.row, first), self.shift(self.col, second)

    def neighbour(self, half, axis, sgn):
        if (axis == 0) == (half == 0):
            row, col = self.row, self.shift(self.col, sgn)
        else:
            row, col = self.shift(self.row, sgn), self.col
        return self.member(row, col)

    def member(self, row, col):
        return {'tp': (row * self.side + col) * 2 + self.core}

    def partner(self):
        return {'tp': (self.row * self.side + self.col) * 2 + (1 - self.core)}

    def pair_copy(self, src, dst, send_sem, recv_sem, num):
        return pltpu.make_async_remote_copy(src_ref=src, dst_ref=dst, send_sem=send_sem.at[num], recv_sem=recv_sem.at[num],
                                            device_id=self.partner(), device_id_type=MESH)

    def barrier(self, with_partner=False):
        sem = pltpu.get_barrier_semaphore()
        targets = [self.neighbour(half, 0, sgn) for half in PAIR for sgn in WAYS] + [self.partner()] * with_partner
        for target in targets:
            pl.semaphore_signal(sem, inc=1, device_id=target, device_id_type=MESH)
        pl.semaphore_wait(sem, len(targets))


class Gather:
    def __init__(self, net, buf, send_sem, recv_sem, rows, start=0):
        self.net, self.buf, self.send_sem, self.recv_sem = net, buf, send_sem, recv_sem
        self.rows, self.base = rows, start
        self.sent = []

    def ident(self, half, stage, first, kind):
        return half * 20 + (0 if stage == 0 else 4 + 4 * OFFS.index(first)) + kind

    def slot(self, half, first, second, kind):
        row, col = self.net.block(half, first, second)
        n_half = self.rows // 2
        start, size = self.base + half * n_half, n_half
        if kind >= 2:
            size = n_half // 2
            start += (kind - 2) * size
        return self.buf.at[row, col, pl.ds(start, size)]

    def copy(self, half, stage, first, kind, ref):
        ident = self.ident(half, stage, first, kind)
        sgn = 1 if kind % 2 == 0 else -1
        return pltpu.make_async_remote_copy(
            src_ref=ref, dst_ref=ref, send_sem=self.send_sem.at[ident], recv_sem=self.recv_sem.at[ident],
            device_id=self.net.neighbour(half, stage, sgn), device_id_type=MESH)

    def send(self, half, stage, first, kind):
        back = (0, 0, -1, 1)[kind]
        offs = (back, 0) if stage == 0 else (first, back)
        copy = self.copy(half, stage, first, kind, self.slot(half, offs[0], offs[1], kind))
        copy.start()
        self.sent.append(copy)

    def wait(self, half, stage, first, kind):
        back = (-1, 1, 2, 2)[kind]
        offs = (back, 0) if stage == 0 else (first, back)
        self.copy(half, stage, first, kind, self.slot(half, offs[0], offs[1], kind)).wait_recv()

    def each(self, call, stage, first, kinds):
        for kind in kinds:
            for half in PAIR:
                call(half, stage, first, kind)

    def onward(self, half, stage, first, kind):
        self.wait(half, stage, first, kind)
        self.send(half, stage, first, kind + 2)

    def steps(self):
        self.each(self.send, 0, 0, PAIR)
        self.each(self.send, 1, 0, PAIR)
        yield
        for kind in PAIR:
            for half in PAIR:
                self.onward(half, 0, 0, kind)
                for way in PAIR:
                    self.send(half, 1, -WAYS[kind], way)
        yield
        self.each(self.onward, 1, 0, PAIR)
        yield
        self.each(self.wait, 0, 0, LATE)
        self.each(self.send, 1, 2, PAIR)
        yield
        for first in OFFS[1:]:
            self.each(self.onward, 1, first, PAIR)
            yield
        for first in OFFS:
            self.each(self.wait, 1, first, LATE)
        for copy in self.sent:
            copy.wait_send()


class Scatter:
    def __init__(self, net, part, recv, out, held, last, send_sem, recv_sem, start=0):
        self.net, self.part, self.recv, self.out, self.held, self.last = net, part, recv, out, held, last
        self.send_sem, self.recv_sem = send_sem, recv_sem
        self.quarter, self.base = recv.shape[-2], start
        self.sent = []

    def copy(self, half, stage, way, kind, ref):
        ident = ((half * 5 + stage) * 2 + way) * 3 + kind
        return pltpu.make_async_remote_copy(
            src_ref=ref, dst_ref=self.recv.at[half, stage, way, kind],
            send_sem=self.send_sem.at[ident], recv_sem=self.recv_sem.at[ident],
            device_id=self.net.neighbour(half, 0 if stage == 4 else 1, WAYS[way]), device_id_type=MESH)

    def send(self, half, stage, way, kind, ref):
        copy = self.copy(half, stage, way, kind, ref)
        copy.start()
        self.sent.append(copy)

    def wait(self, half, stage, way, kind):
        self.copy(half, stage, way, kind, self.recv.at[half, stage, way, kind]).wait_recv()

    def term(self, half, stage, off, sub):
        if stage == 4:
            return self.held.at[half, {2: 0, 1: 1, -1: 2}[off], pl.ds(sub * self.quarter, self.quarter)]
        row, col = self.net.block(half, RS_ORDER[stage], off)
        return self.part.at[row, col, pl.ds(self.base + (2 * half + sub) * self.quarter, self.quarter)]

    def far(self, half, stage):
        for way in PAIR:
            self.send(half, stage, way, 0, self.term(half, stage, 2, way))

    def near_plain(self, half, stage, way):
        self.send(half, stage, way, 1, self.term(half, stage, WAYS[way], 1 - way))

    def near_summed(self, half, stage, way):
        self.wait(half, stage, way, 0)
        total = self.term(half, stage, WAYS[way], way)[...].astype(F32) + self.recv[half, stage, way, 0].astype(F32)
        self.out[half, stage, way] = total.astype(BF)
        self.send(half, stage, way, 2, self.out.at[half, stage, way])

    def arrived(self, half, stage, sub):
        first = self.recv[half, stage, 0, 2 if sub == 0 else 1].astype(F32)
        second = self.recv[half, stage, 1, 1 if sub == 0 else 2].astype(F32)
        return first + second

    def finish(self, half, stage):
        for way in PAIR:
            self.wait(half, stage, way, 1)
            self.wait(half, stage, way, 2)
        for sub in PAIR:
            total = self.term(half, stage, 0, sub)[...].astype(F32) + self.arrived(half, stage, sub)
            rows = pl.ds(sub * self.quarter, self.quarter)
            if stage < 3:
                self.held[half, stage, rows] = total.astype(BF)
            else:
                self.last[half, rows] = total

    def near(self, stage):
        for half in PAIR:
            for way in PAIR:
                self.near_summed(half, stage, way)
                self.near_plain(half, stage, way)

    def steps(self):
        last = len(OFFS)
        for stage in range(last):
            for half in PAIR:
                self.far(half, stage)
        yield
        for stage in range(last - 1):
            self.near(stage)
            yield
        for half in PAIR:
            self.finish(half, 0)
            self.far(half, last)
        yield
        self.near(last - 1)
        yield
        for stage in (1, 2):
            for half in PAIR:
                self.finish(half, stage)
                self.near_plain(half, last, stage - 1)
        yield
        for half in PAIR:
            for way in PAIR:
                self.near_summed(half, last, way)
        yield
        for half in PAIR:
            self.finish(half, last - 1)
        yield
        for half in PAIR:
            for way in PAIR:
                self.wait(half, last, way, 1)
                self.wait(half, last, way, 2)
            for sub in PAIR:
                rows = pl.ds(sub * self.quarter, self.quarter)
                self.last[half, rows] = self.last[half, rows] + self.arrived(half, last, sub)
        for copy in self.sent:
            copy.wait_send()

    def total(self):
        n_half, width = self.last.shape[1:]
        return self.last[...].reshape(2 * n_half, width)


def exchanged(net, part_ref, out_ref, scratch, middle, other, order):
    scatter = Scatter(net, part_ref, *scratch[:6])
    tasks = {'a': scatter.steps(), 'x': other}
    if out_ref is not None:
        tasks['c'] = Gather(net, out_ref, *scratch[6:], part_ref.shape[2]).steps()
    for code in order:
        if code == 'm':
            for _ in tasks['a']:
                pass
            middle(scatter.total())
        else:
            next(tasks[code], None)
    for task in tasks.values():
        for _ in task:
            pass


def weight_work(net, jobs, send_sem, recv_sem):
    def product(job, which, store):
        left, right, split_left, out = job[:4]
        count = out.shape[0] if split_left else out.shape[1]
        own = slice(which * count, (which + 1) * count)
        wide = right.shape[1] if split_left else left.shape[1]

        def chunk(num, carry):
            cols = pl.ds(pl.multiple_of(num * WORK_CHUNK, WORK_CHUNK), WORK_CHUNK)
            if split_left:
                store((slice(None), cols), matmul(left[:, own], right[:, cols], TN))
            else:
                store((cols, slice(None)), matmul(left[:, cols], right[:, own], TN))
            return carry

        lax.fori_loop(0, wide // WORK_CHUNK, chunk, 0)

    copies = []
    for num, job in enumerate(jobs):
        def keep(place, vals, send=job[4]):
            send[place] = vals.astype(BF)
        product(job, 1, keep)
        copies.append(net.pair_copy(job[4], job[5], send_sem, recv_sem, num))
        copies[-1].start()
        yield
    for copy, job in zip(copies, jobs):
        copy.wait_recv()

        def add(place, vals, out=job[3], recv=job[5]):
            out[place] = (vals + recv[place].astype(F32)).astype(BF)
        product(job, 0, add)
        yield
    for copy in copies:
        copy.wait_send()


def gather_scratch():
    return [pltpu.SemaphoreType.DMA((40,)), pltpu.SemaphoreType.DMA((40,))]


def scatter_scratch(rows, width):
    quarter = rows // 4
    return [pltpu.VMEM((2, 5, 2, 3, quarter, width), BF),
            pltpu.VMEM((2, 5, 2, quarter, width), BF),
            pltpu.VMEM((2, 3, 2 * quarter, width), BF),
            pltpu.VMEM((2, 2 * quarter, width), F32),
            pltpu.SemaphoreType.DMA((60,)), pltpu.SemaphoreType.DMA((60,))]


def vmem_specs(count):
    return [pl.BlockSpec(memory_space=pltpu.VMEM)] * count


def comm_params(ident):
    return pltpu.CompilerParams(collective_id=ident, has_side_effects=True, vmem_limit_bytes=COMM_VMEM[ident])


def normalised(vals):
    mean_val = jnp.mean(vals, axis=-1, keepdims=True)
    centered = vals - mean_val
    var_val = jnp.mean(centered * centered, axis=-1, keepdims=True)
    inv_std = lax.rsqrt(var_val + LN_EPS)
    return centered * inv_std, inv_std


def norm_backward(d_out, vals, gain):
    unit, inv_std = normalised(vals)
    d_unit = d_out * gain
    mean_d = jnp.mean(d_unit, axis=-1, keepdims=True)
    mean_du = jnp.mean(d_unit * unit, axis=-1, keepdims=True)
    d_vals = inv_std * (d_unit - mean_d - unit * mean_du)
    return d_vals, jnp.sum(d_out * unit, axis=0, keepdims=True), jnp.sum(d_out, axis=0, keepdims=True)


def col_sum(vals):
    return jnp.sum(vals, axis=0, keepdims=True)


def first_kernel(group_size, x_ref, par_ref, h_ref, g_send, g_recv):
    net = Net(group_size)
    unit, _ = normalised(x_ref[...].astype(F32))
    h_ref[net.row, net.col] = (unit * par_ref[0:1] + par_ref[1:2]).astype(BF)
    net.barrier()
    for _ in Gather(net, h_ref, g_send, g_recv, x_ref.shape[0]).steps():
        pass


def forward_kernel(group_size, part_ref, res_ref, par_ref, new_ref, h_ref, *scratch):
    net = Net(group_size)
    net.barrier()

    def middle(total):
        new = res_ref[...] + total + par_ref[0:1]
        new_ref[...] = new
        unit, _ = normalised(new)
        h_ref[net.row, net.col] = (unit * par_ref[1:2] + par_ref[2:3]).astype(BF)

    exchanged(net, part_ref, h_ref, scratch, middle, iter(PAIR), BOTH_ORDER)


def backward_kernel(splits, gathers, group_size, part_ref, res_ref, par_ref, dres_ref, *refs):
    net = Net(group_size)
    net.barrier(True)
    work, refs = refs[:4], refs[4:]
    outs, refs = refs[:2], refs[2:]
    new_ref, sum_ref = refs[:2]
    d_ref = refs[2] if gathers else None
    bufs = refs[3 if gathers else 2:]
    jobs = [(work[2 * num], work[2 * num + 1], split, outs[num], bufs[2 * num], bufs[2 * num + 1]) for num, split in enumerate(splits)]
    send_sem, recv_sem = bufs[4:6]

    def middle(total):
        d_vals, d_gain, d_shift = norm_backward(total, res_ref[...], par_ref[0:1])
        new = dres_ref[...] + d_vals
        new_ref[...] = new.astype(new_ref.dtype)
        if gathers:
            d_ref[net.row, net.col] = new.astype(BF)
        sum_ref[0:1] = d_gain
        sum_ref[1:2] = d_shift
        sum_ref[2:3] = col_sum(new)

    exchanged(net, part_ref, d_ref, bufs[6:], middle, weight_work(net, jobs, send_sem, recv_sem), BOTH_ORDER if gathers else SCATTER_ORDER)


def sum_kernel(group_size, in_ref, out_ref, buf, pair_buf, sem_s, sem_r):
    net = Net(group_size)
    sem = pltpu.get_barrier_semaphore()
    far = range(1, net.side)
    devs = [[net.member(net.row, net.shift(net.col, off)) for off in far], [net.member(net.shift(net.row, off), net.col) for off in far]]
    everyone = devs[0] + devs[1] + [net.partner()]
    for dev in everyone:
        pl.semaphore_signal(sem, inc=1, device_id=dev, device_id_type=MESH)
    pl.semaphore_wait(sem, len(everyone))
    n_half = in_ref.shape[0] // 2
    own, other = [pl.ds(pl.multiple_of(core * n_half, n_half), n_half) for core in (net.core, 1 - net.core)]
    copy = net.pair_copy(in_ref.at[other], pair_buf, sem_s, sem_r, 0)
    copy.start()
    copy.wait()
    value = in_ref[own] + pair_buf[...]
    for axis in PAIR:
        place = net.row if axis else net.col
        buf[axis, place] = value
        copies = []
        for num, dev in enumerate(devs[axis]):
            ident = 2 + axis * len(far) + num
            copies.append(pltpu.make_async_remote_copy(
                src_ref=buf.at[axis, place], dst_ref=buf.at[axis, place], send_sem=sem_s.at[ident], recv_sem=sem_r.at[ident],
                device_id=dev, device_id_type=MESH))
            copies[-1].start()
        for copy in copies:
            copy.wait_recv()
        value = sum(buf[axis, num] for num in range(net.side))
        for copy in copies:
            copy.wait_send()
    out_ref[own] = value
    copy = net.pair_copy(out_ref.at[own], out_ref.at[own], sem_s, sem_r, 1)
    copy.start()
    copy.wait()


def gelu_tanh(pre_act):
    return jax.nn.gelu(pre_act, approximate=True)


def attention_kernel(group_size, qkv_ref, dy_ref, nat_ref, stat_ref, a_ref, plane_ref, send, score, prob, a_nat, a_part, send_sem, recv_sem, g_send, g_recv):
    net = Net(group_size)
    plane_ref[net.row, net.col] = dy_ref[...]
    net.barrier(True)
    moves = Gather(net, plane_ref, g_send, g_recv, dy_ref.shape[0]).steps()
    parts, n_blk, _, rows, head = nat_ref.shape
    core, n_plane = net.core, n_blk * rows
    for part in range(parts):
        send[part] = qkv_ref[:, (parts + part) * head:(parts + part + 1) * head].reshape(n_blk, rows, head)
    copies = [net.pair_copy(send, nat_ref.at[:, :, core], send_sem, recv_sem, 0)]
    copies[0].start()
    next(moves)
    for part in range(parts):
        nat_ref[part, :, core] = qkv_ref[:, part * head:(part + 1) * head].reshape(n_blk, rows, head)
    copies[0].wait_recv()
    step = n_blk // Q_BLOCKS
    n_q = 2 * step * rows
    factor = head ** -0.5 * LOG2E
    for blk in reversed(range(Q_BLOCKS)):
        here, upto, left = pl.ds(blk * step, step), (blk + 1) * step, blk * n_q
        size = left + n_q
        score[:, :size] = matmul(nat_ref[0, here].reshape(n_q, head), nat_ref[1, :upto].reshape(size, head), NT)

        def softmax_rows(num, carry):
            row = pl.ds(pl.multiple_of(num * ROW_CHUNK, ROW_CHUNK), ROW_CHUNK)
            vals = [score[row, :left]] if left else []
            vals.append(masked(score[row, left:size], num * ROW_CHUNK))
            top = functools.reduce(jnp.maximum, [jnp.max(val, axis=1, keepdims=True) for val in vals])
            exps = [jnp.exp2((val - top) * factor) for val in vals]
            inv = 1.0 / sum(jnp.sum(val, axis=1, keepdims=True) for val in exps)
            if left:
                prob[row, :left] = (exps[0] * inv).astype(BF)
            prob[row, left:size] = (exps[-1] * inv).astype(BF)
            stat = pl.ds(pl.multiple_of(left + num * ROW_CHUNK, ROW_CHUNK), ROW_CHUNK)
            stat_ref[0, stat] = top
            stat_ref[1, stat] = inv
            return carry

        lax.fori_loop(0, n_q // ROW_CHUNK, softmax_rows, 0, unroll=ROW_UNROLL)
        attn = matmul(prob[:, :size], nat_ref[2, :upto].reshape(size, head), NN).astype(BF)
        a_nat[here] = attn.reshape(step, 2, rows, head)
        copies.append(net.pair_copy(a_nat.at[here, 1 - core], a_part.at[here], send_sem, recv_sem, 1 + blk))
        copies[-1].start()
        for _ in range(GATHER_PLAN[Q_BLOCKS - 1 - blk]):
            next(moves, None)
    a_ref[:, :head] = a_nat[:, core].reshape(n_plane, head)
    for copy in copies[1:]:
        copy.wait_recv()
    a_ref[:, head:] = a_part[...].reshape(n_plane, head)
    for _ in moves:
        pass
    for copy in copies:
        copy.wait_send()


def masked(vals, first_row):
    row = first_row + lax.broadcasted_iota(jnp.int32, vals.shape, 0)
    return jnp.where(row >= lax.broadcasted_iota(jnp.int32, vals.shape, 1), vals, -1e30)


def attention_back_kernel(first_row, group_size, d_ref, nat_ref, stat_ref, part_ref, res_ref, bias_ref, dq_ref, y_ref, send, d_nat, score, d_prob, prob, d_score, dk_acc, dv_acc,
                          g_nat, g_part, send_sem, recv_sem, *scratch):
    net = Net(group_size)
    net.barrier(True)
    scatter = Scatter(net, part_ref, *scratch, start=first_row)
    moves = scatter.steps()
    parts, n_blk, _, rows, head = nat_ref.shape
    core, n_plane = net.core, n_blk * rows
    send[...] = d_ref[:, head:].reshape(n_blk, rows, head)
    copies = [net.pair_copy(send, d_nat.at[:, core], send_sem, recv_sem, 0)]
    copies[0].start()
    next(moves)
    d_nat[:, core] = d_ref[:, :head].reshape(n_blk, rows, head)
    copies[0].wait_recv()
    step = n_blk // Q_BLOCKS
    n_q = 2 * step * rows
    scale = head ** -0.5
    for blk in reversed(range(Q_BLOCKS)):
        here, upto, left = pl.ds(blk * step, step), (blk + 1) * step, blk * n_q
        size = left + n_q
        q_vals = nat_ref[0, here].reshape(n_q, head)
        k_vals = nat_ref[1, :upto].reshape(size, head)
        d_vals = d_nat[here].reshape(n_q, head)
        score[:, :size] = matmul(q_vals, k_vals, NT)
        d_prob[:, :size] = matmul(d_vals, nat_ref[2, :upto].reshape(size, head), NT)

        def score_rows(num, carry):
            row = pl.ds(pl.multiple_of(num * BACK_CHUNK, BACK_CHUNK), BACK_CHUNK)
            stat = pl.ds(pl.multiple_of(left + num * BACK_CHUNK, BACK_CHUNK), BACK_CHUNK)
            top, inv = stat_ref[0, stat], stat_ref[1, stat]
            cols = [slice(0, left)] if left else []
            cols.append(slice(left, size))
            probs = []
            for col in cols:
                val = score[row, col]
                if col is cols[-1]:
                    val = masked(val, num * BACK_CHUNK)
                probs.append((jnp.exp2((val - top) * (scale * LOG2E)) * inv).astype(BF))
                prob[row, col] = probs[-1]
            wide = [val.astype(F32) for val in probs]
            grads = [d_prob[row, col] for col in cols]
            dot = sum(jnp.sum(val * grad, axis=1, keepdims=True) for val, grad in zip(wide, grads))
            for col, val, grad in zip(cols, wide, grads):
                d_score[row, col] = (val * (grad - dot) * scale).astype(BF)
            return carry

        lax.fori_loop(0, n_q // BACK_CHUNK, score_rows, 0, unroll=BACK_UNROLL)
        g_nat[0, here] = matmul(d_score[:, :size], k_vals, NN).astype(BF).reshape(step, 2, rows, head)
        for acc, lhs, rhs in ((dk_acc, d_score, q_vals), (dv_acc, prob, d_vals)):
            term = matmul(lhs[:, :size], rhs, TN)
            if blk + 1 == Q_BLOCKS:
                acc[...] = term
            else:
                acc[:size] = acc[:size] + term
        for part, acc in ((1, dk_acc), (2, dv_acc)):
            g_nat[part, here] = acc[left:size].astype(BF).reshape(step, 2, rows, head)
        copies.append(net.pair_copy(g_nat.at[:, here, 1 - core], g_part.at[:, here], send_sem, recv_sem, 1 + blk))
        copies[-1].start()
        next(moves, None)
    for part in range(parts):
        dq_ref[:, part * head:(part + 1) * head] = g_nat[part, :, core].reshape(n_plane, head)
    for copy in copies[1:]:
        copy.wait_recv()
    for part in range(parts):
        dq_ref[:, (parts + part) * head:(parts + part + 1) * head] = g_part[part].reshape(n_plane, head)
    for _ in moves:
        pass
    y_ref[...] = (res_ref[...] + scatter.total() + bias_ref[...]).astype(BF)
    for copy in copies:
        copy.wait_send()


def solution(mesh):
    group_size = mesh.shape['tp']
    side = math.isqrt(group_size // 2)
    if 2 * side * side != group_size or side != len(OFFS):
        raise ValueError('unsupported group')
    swap = [(dev, dev + 1 - 2 * (dev % 2)) for dev in range(group_size)]

    def device_step(x_loc, dy_loc, ln_par, bias_d, w_qkv, w_out, w_up, b_up, w_down):
        n_layers, width = ln_par.shape[0], x_loc.shape[-1]
        rows = x_loc.shape[1]
        n_plane = rows * side * side
        head = w_qkv.shape[-1]
        n_col = w_up.shape[-1]
        plane = jax.ShapeDtypeStruct((side, side, rows, width), BF)
        local_f = jax.ShapeDtypeStruct((rows, width), F32)
        local_b = jax.ShapeDtypeStruct((rows, width), BF)

        def sums(count):
            return jax.ShapeDtypeStruct((count, width), F32)

        def comm(kernel, ident, args, outs, scratch, *static):
            return pl.pallas_call(
                functools.partial(kernel, *static, group_size), name=kernel.__name__, out_shape=outs,
                in_specs=vmem_specs(len(args)), out_specs=jax.tree.map(lambda _: vmem_specs(1)[0], outs),
                scratch_shapes=scratch, compiler_params=comm_params(ident))(*args)

        block_shape = (side * side, rows, head)
        nat_shape = jax.ShapeDtypeStruct((3, side * side, 2, rows, head), BF)
        n_all, n_q = 2 * n_plane, 2 * n_plane // Q_BLOCKS
        stat_shape = jax.ShapeDtypeStruct((2, n_all, 1), F32)
        pair_sems = [pltpu.SemaphoreType.DMA((1 + Q_BLOCKS,))] * 2

        part_rows = rows // n_layers
        part_scatter = scatter_scratch(part_rows, width)
        one_scatter = scatter_scratch(rows, width)
        both_scratch = one_scatter + gather_scratch()

        def part_slice(layer):
            return slice(layer * part_rows, (layer + 1) * part_rows)

        def swapped(vals):
            return lax.ppermute(vals, 'tp', swap)

        def blocks(part):
            return part.astype(BF).reshape(side, side, rows, width)

        wq_mine = w_qkv.reshape(n_layers, width, 3 * head)
        wq_both = jnp.concatenate([wq_mine, swapped(wq_mine)], axis=2)
        wo_mine = w_out.reshape(n_layers, head, width)
        wo_both = jnp.concatenate([wo_mine, swapped(wo_mine)], axis=1)
        wu_both = jnp.concatenate([w_up, swapped(w_up)], axis=2)
        wd_both = jnp.concatenate([w_down, swapped(w_down)], axis=1)
        bu_both = jnp.concatenate([b_up, swapped(b_up)], axis=1)

        x_rows = x_loc.reshape(rows, width)
        dy_rows = dy_loc.reshape(rows, width)
        h_plane = comm(first_kernel, 0, [x_rows, ln_par[0, 0:2]], plane, gather_scratch())
        res_one = x_rows.astype(F32)
        saved, d_parts, y_parts = [], [], [None] * n_layers
        for layer in range(n_layers):
            h_flat = h_plane.reshape(n_plane, width)
            qkv = matmul(h_flat, wq_both[layer], NN).astype(BF)
            nat, stat, a_both, dy_part = comm(attention_kernel, 6, [qkv, dy_rows[part_slice(layer)]], (
                nat_shape, stat_shape, jax.ShapeDtypeStruct((n_plane, 2 * head), BF), jax.ShapeDtypeStruct((side, side, part_rows, width), BF)), [
                pltpu.VMEM((3,) + block_shape, BF), pltpu.VMEM((n_q, n_all), F32), pltpu.VMEM((n_q, n_all), BF),
                pltpu.VMEM(nat_shape.shape[1:], BF), pltpu.VMEM(block_shape, BF)] + pair_sems + gather_scratch())
            d_parts.append(dy_part)
            part = blocks(matmul(a_both, wo_both[layer], NN))
            par = jnp.concatenate([bias_d[layer, 0:1], ln_par[layer, 2:4]], axis=0)
            res_two, h2_plane = comm(forward_kernel, 1, [part, res_one, par], (local_f, plane), both_scratch)
            h2_flat = h2_plane.reshape(n_plane, width)
            pre_act = matmul(h2_flat, wu_both[layer], NN) + bu_both[layer]
            act_f, gelu_pull = jax.vjp(gelu_tanh, pre_act)
            act = act_f.astype(BF)
            part = blocks(matmul(act, wd_both[layer], NN))
            saved.append((res_one, h_flat, nat, stat, a_both, res_two, h2_flat, gelu_pull, act))
            if layer + 1 < n_layers:
                par = jnp.concatenate([bias_d[layer, 1:2], ln_par[layer + 1, 0:2]], axis=0)
                res_one, h_plane = comm(forward_kernel, 1, [part, res_two, par], (local_f, plane), both_scratch)

        top_part, top_res = part, res_two
        d_plane = jnp.concatenate(d_parts, axis=2)
        def backward(args, splits, shapes, ident, gathers):
            outs = [jax.ShapeDtypeStruct(shape, BF) for shape in shapes] + [local_f if gathers else local_b, sums(3)] + [plane] * gathers
            bufs = [pltpu.VMEM(shape, BF) for shape in shapes for _ in PAIR] + [pltpu.SemaphoreType.DMA((2,))] * 2
            return comm(backward_kernel, ident, args, tuple(outs), bufs + one_scatter + gather_scratch() * gathers, splits, gathers)

        d_res = dy_rows.astype(F32)
        bias_two = jnp.sum(d_res, axis=0, keepdims=True)
        grads = [None] * n_layers
        for layer in reversed(range(n_layers)):
            res_one, h_flat, nat, stat, a_both, res_two, h2_flat, gelu_pull, act = saved[layer]
            d_flat = d_plane.reshape(n_plane, width)
            d_act = matmul(d_flat, wd_both[layer], NT)
            d_pre = gelu_pull(d_act)[0]
            d_pre_bf = d_pre.astype(BF)
            d_bup = jnp.sum(d_pre, axis=0)
            part = blocks(matmul(d_pre_bf, wu_both[layer], NT))
            d_wdown, d_wup, d_res, sum_two, da_plane = backward(
                [part, res_two, ln_par[layer, 2:3], d_res, act, d_flat, h2_flat, d_pre_bf], (True, False),
                [(n_col, width), (width, n_col)], 3, True)
            da_flat = da_plane.reshape(n_plane, width)
            d_both = matmul(da_flat, wo_both[layer], NT).astype(BF)
            dq_both, y_part = comm(attention_back_kernel, 7 + layer, [d_both, nat, stat, top_part, top_res[part_slice(layer)], bias_d[n_layers - 1, 1:2]], (
                jax.ShapeDtypeStruct((n_plane, 6 * head), BF), jax.ShapeDtypeStruct((part_rows, width), BF)), [
                pltpu.VMEM(block_shape, BF), pltpu.VMEM(nat_shape.shape[1:], BF), pltpu.VMEM((n_q, n_all), F32),
                pltpu.VMEM((n_q, n_all), F32), pltpu.VMEM((n_q, n_all), BF), pltpu.VMEM((n_q, n_all), BF),
                pltpu.VMEM((n_all, head), F32), pltpu.VMEM((n_all, head), F32), pltpu.VMEM(nat_shape.shape, BF),
                pltpu.VMEM((3,) + block_shape, BF)] + pair_sems + part_scatter, layer * part_rows)
            y_parts[layer] = y_part
            part = blocks(matmul(dq_both, wq_both[layer], NT))
            args = [part, res_one, ln_par[layer, 0:1], d_res, a_both, da_flat, h_flat, dq_both]
            shapes = [(head, width), (width, 3 * head)]
            if layer > 0:
                d_wout, d_wqkv, d_res, sum_one, d_plane = backward(args, (True, False), shapes, 4, True)
            else:
                d_wout, d_wqkv, x_grad, sum_one = backward(args, (True, False), shapes, 5, False)
            next_two = sum_one[2:3]
            small = jnp.concatenate([sum_one[0:2], sum_two[0:2], sum_two[2:3], bias_two], axis=0)
            bias_two = next_two
            grads[layer] = (small, d_wqkv, d_wout, d_wup, d_bup[:n_col] + swapped(d_bup[n_col:]), d_wdown)
        n_small = grads[0][0].shape[0]
        packed = jnp.concatenate([grad[0] for grad in grads], axis=0)
        pad = -packed.shape[0] % 16
        packed = jnp.concatenate([packed, jnp.zeros((pad, width), F32)], axis=0)
        half_shape = (packed.shape[0] // 2, width)
        total = comm(sum_kernel, 2, [packed], sums(packed.shape[0]),
                     [pltpu.VMEM((2, side) + half_shape, F32), pltpu.VMEM(half_shape, F32)] + [pltpu.SemaphoreType.DMA((2 * side,))] * 2)
        total = total[:n_small * n_layers].reshape(n_layers, n_small, width)
        return (jnp.concatenate(y_parts, axis=0).reshape(x_loc.shape), x_grad.reshape(x_loc.shape), total[:, :4], total[:, 4:],
                jnp.stack([grad[1].reshape(width, 3, 1, head) for grad in grads]),
                jnp.stack([grad[2].reshape(1, head, width) for grad in grads]),
                jnp.stack([grad[3] for grad in grads]),
                jnp.stack([grad[4] for grad in grads]),
                jnp.stack([grad[5] for grad in grads]))

    def on_tp(dim, first=None):
        return P(first, *[None] * (dim - 1), 'tp')

    rows_spec = P('dp', 'tp')
    in_specs = (rows_spec, rows_spec, P(), P(), on_tp(3), on_tp(1), on_tp(2), on_tp(1), on_tp(1))
    out_specs = (rows_spec, rows_spec, P('dp'), P('dp'), on_tp(3, 'dp'), on_tp(1, 'dp'), on_tp(2, 'dp'), on_tp(1, 'dp'), on_tp(1, 'dp'))
    return jax.shard_map(device_step, mesh=mesh, in_specs=in_specs, out_specs=out_specs, check_vma=False)
```

```python
import functools
import math

import jax
import jax.numpy as jnp
from jax import lax
from jax.experimental import pallas as pl
from jax.experimental.pallas import tpu as pltpu
from jax.sharding import PartitionSpec as P

MESH = pl.DeviceIdType.MESH
BF = jnp.bfloat16
F32 = jnp.float32
LN_EPS = 1e-5
OFFS = (0, -1, 1, 2)
RS_ORDER = (2, 1, -1, 0)
PAIR = (0, 1)
WAYS = (1, -1)
LATE = (2, 3)
NN = ((1,), (0,))
NT = ((1,), (1,))
TN = ((0,), (0,))
MIB = 1 << 20
COMM_VMEM = [size * MIB for size in (4, 10, 6, 16, 14, 14, 12, 20, 20)]
Q_BLOCKS = 8
ROW_CHUNK = 64
BACK_CHUNK = 64
ROW_UNROLL = 4
BACK_UNROLL = 2
LOG2E = math.log2(math.e)
BOTH_ORDER = 'axaaaxaaaaaamccxccxcccc'
SCATTER_ORDER = 'axaxaaxaaxaaam'
WORK_CHUNK = 512
COST = pl.CostEstimate(flops=20 * 10 ** 9, bytes_accessed=MIB, transcendentals=0)
GATHER_PLAN = [int(code) for code in '01011111']


def matmul(lhs, rhs, dims):
    return lax.dot_general(lhs, rhs, (dims, ((), ())), preferred_element_type=F32)


class Net:
    def __init__(self, group_size):
        side = math.isqrt(group_size // 2)
        me = lax.axis_index('tp')
        self.side = side
        self.core = lax.rem(me, 2)
        self.col = lax.rem(me // 2, side)
        self.row = me // (2 * side)

    def shift(self, pos, off):
        return lax.rem(pos + (off + self.side), self.side)

    def block(self, half, first, second):
        if half == 0:
            return self.shift(self.row, second), self.shift(self.col, first)
        return self.shift(self.row, first), self.shift(self.col, second)

    def neighbour(self, half, axis, sgn):
        if (axis == 0) == (half == 0):
            row, col = self.row, self.shift(self.col, sgn)
        else:
            row, col = self.shift(self.row, sgn), self.col
        return self.member(row, col)

    def member(self, row, col):
        return {'tp': (row * self.side + col) * 2 + self.core}

    def partner(self):
        return {'tp': (self.row * self.side + self.col) * 2 + (1 - self.core)}

    def pair_copy(self, src, dst, send_sem, recv_sem, num):
        return pltpu.make_async_remote_copy(src_ref=src, dst_ref=dst, send_sem=send_sem.at[num], recv_sem=recv_sem.at[num],
                                            device_id=self.partner(), device_id_type=MESH)

    def barrier(self, with_partner=False):
        sem = pltpu.get_barrier_semaphore()
        targets = [self.neighbour(half, 0, sgn) for half in PAIR for sgn in WAYS] + [self.partner()] * with_partner
        for target in targets:
            pl.semaphore_signal(sem, inc=1, device_id=target, device_id_type=MESH)
        pl.semaphore_wait(sem, len(targets))


class Gather:
    def __init__(self, net, buf, send_sem, recv_sem, rows, start=0):
        self.net, self.buf, self.send_sem, self.recv_sem = net, buf, send_sem, recv_sem
        self.rows, self.base = rows, start
        self.sent = []

    def ident(self, half, stage, first, kind):
        return half * 20 + (0 if stage == 0 else 4 + 4 * OFFS.index(first)) + kind

    def slot(self, half, first, second, kind):
        row, col = self.net.block(half, first, second)
        n_half = self.rows // 2
        start, size = self.base + half * n_half, n_half
        if kind >= 2:
            size = n_half // 2
            start += (kind - 2) * size
        return self.buf.at[row, col, pl.ds(start, size)]

    def copy(self, half, stage, first, kind, ref):
        ident = self.ident(half, stage, first, kind)
        sgn = 1 if kind % 2 == 0 else -1
        return pltpu.make_async_remote_copy(
            src_ref=ref, dst_ref=ref, send_sem=self.send_sem.at[ident], recv_sem=self.recv_sem.at[ident],
            device_id=self.net.neighbour(half, stage, sgn), device_id_type=MESH)

    def send(self, half, stage, first, kind):
        back = (0, 0, -1, 1)[kind]
        offs = (back, 0) if stage == 0 else (first, back)
        copy = self.copy(half, stage, first, kind, self.slot(half, offs[0], offs[1], kind))
        copy.start()
        self.sent.append(copy)

    def wait(self, half, stage, first, kind):
        back = (-1, 1, 2, 2)[kind]
        offs = (back, 0) if stage == 0 else (first, back)
        self.copy(half, stage, first, kind, self.slot(half, offs[0], offs[1], kind)).wait_recv()

    def each(self, call, stage, first, kinds):
        for kind in kinds:
            for half in PAIR:
                call(half, stage, first, kind)

    def onward(self, half, stage, first, kind):
        self.wait(half, stage, first, kind)
        self.send(half, stage, first, kind + 2)

    def steps(self):
        self.each(self.send, 0, 0, PAIR)
        self.each(self.send, 1, 0, PAIR)
        yield
        for kind in PAIR:
            for half in PAIR:
                self.onward(half, 0, 0, kind)
                for way in PAIR:
                    self.send(half, 1, -WAYS[kind], way)
        yield
        self.each(self.onward, 1, 0, PAIR)
        yield
        self.each(self.wait, 0, 0, LATE)
        self.each(self.send, 1, 2, PAIR)
        yield
        for first in OFFS[1:]:
            self.each(self.onward, 1, first, PAIR)
            yield
        for first in OFFS:
            self.each(self.wait, 1, first, LATE)
        for copy in self.sent:
            copy.wait_send()


class Scatter:
    def __init__(self, net, part, recv, out, held, last, send_sem, recv_sem, start=0):
        self.net, self.part, self.recv, self.out, self.held, self.last = net, part, recv, out, held, last
        self.send_sem, self.recv_sem = send_sem, recv_sem
        self.quarter, self.base = recv.shape[-2], start
        self.sent = []

    def copy(self, half, stage, way, kind, ref):
        ident = ((half * 5 + stage) * 2 + way) * 3 + kind
        return pltpu.make_async_remote_copy(
            src_ref=ref, dst_ref=self.recv.at[half, stage, way, kind],
            send_sem=self.send_sem.at[ident], recv_sem=self.recv_sem.at[ident],
            device_id=self.net.neighbour(half, 0 if stage == 4 else 1, WAYS[way]), device_id_type=MESH)

    def send(self, half, stage, way, kind, ref):
        copy = self.copy(half, stage, way, kind, ref)
        copy.start()
        self.sent.append(copy)

    def wait(self, half, stage, way, kind):
        self.copy(half, stage, way, kind, self.recv.at[half, stage, way, kind]).wait_recv()

    def term(self, half, stage, off, sub):
        if stage == 4:
            return self.held.at[half, {2: 0, 1: 1, -1: 2}[off], pl.ds(sub * self.quarter, self.quarter)]
        row, col = self.net.block(half, RS_ORDER[stage], off)
        return self.part.at[row, col, pl.ds(self.base + (2 * half + sub) * self.quarter, self.quarter)]

    def far(self, half, stage):
        for way in PAIR:
            self.send(half, stage, way, 0, self.term(half, stage, 2, way))

    def near_plain(self, half, stage, way):
        self.send(half, stage, way, 1, self.term(half, stage, WAYS[way], 1 - way))

    def near_summed(self, half, stage, way):
        self.wait(half, stage, way, 0)
        total = self.term(half, stage, WAYS[way], way)[...].astype(F32) + self.recv[half, stage, way, 0].astype(F32)
        self.out[half, stage, way] = total.astype(BF)
        self.send(half, stage, way, 2, self.out.at[half, stage, way])

    def arrived(self, half, stage, sub):
        first = self.recv[half, stage, 0, 2 if sub == 0 else 1].astype(F32)
        second = self.recv[half, stage, 1, 1 if sub == 0 else 2].astype(F32)
        return first + second

    def finish(self, half, stage):
        for way in PAIR:
            self.wait(half, stage, way, 1)
            self.wait(half, stage, way, 2)
        for sub in PAIR:
            total = self.term(half, stage, 0, sub)[...].astype(F32) + self.arrived(half, stage, sub)
            rows = pl.ds(sub * self.quarter, self.quarter)
            if stage < 3:
                self.held[half, stage, rows] = total.astype(BF)
            else:
                self.last[half, rows] = total

    def near(self, stage):
        for half in PAIR:
            for way in PAIR:
                self.near_summed(half, stage, way)
                self.near_plain(half, stage, way)

    def steps(self):
        last = len(OFFS)
        for stage in range(last):
            for half in PAIR:
                self.far(half, stage)
        yield
        for stage in range(last - 1):
            self.near(stage)
            yield
        for half in PAIR:
            self.finish(half, 0)
            self.far(half, last)
        yield
        self.near(last - 1)
        yield
        for stage in (1, 2):
            for half in PAIR:
                self.finish(half, stage)
                self.near_plain(half, last, stage - 1)
        yield
        for half in PAIR:
            for way in PAIR:
                self.near_summed(half, last, way)
        yield
        for half in PAIR:
            self.finish(half, last - 1)
        yield
        for half in PAIR:
            for way in PAIR:
                self.wait(half, last, way, 1)
                self.wait(half, last, way, 2)
            for sub in PAIR:
                rows = pl.ds(sub * self.quarter, self.quarter)
                self.last[half, rows] = self.last[half, rows] + self.arrived(half, last, sub)
        for copy in self.sent:
            copy.wait_send()

    def total(self):
        n_half, width = self.last.shape[1:]
        return self.last[...].reshape(2 * n_half, width)


def exchanged(net, part_ref, out_ref, scratch, middle, other, order):
    scatter = Scatter(net, part_ref, *scratch[:6])
    tasks = {'a': scatter.steps(), 'x': other}
    if out_ref is not None:
        tasks['c'] = Gather(net, out_ref, *scratch[6:], part_ref.shape[2]).steps()
    for code in order:
        if code == 'm':
            for _ in tasks['a']:
                pass
            middle(scatter.total())
        else:
            next(tasks[code], None)
    for task in tasks.values():
        for _ in task:
            pass


def weight_work(net, jobs, send_sem, recv_sem):
    def product(job, which, store):
        left, right, split_left, out = job[:4]
        count = out.shape[0] if split_left else out.shape[1]
        own = slice(which * count, (which + 1) * count)
        wide = right.shape[1] if split_left else left.shape[1]

        def chunk(num, carry):
            cols = pl.ds(pl.multiple_of(num * WORK_CHUNK, WORK_CHUNK), WORK_CHUNK)
            if split_left:
                store((slice(None), cols), matmul(left[:, own], right[:, cols], TN))
            else:
                store((cols, slice(None)), matmul(left[:, cols], right[:, own], TN))
            return carry

        lax.fori_loop(0, wide // WORK_CHUNK, chunk, 0)

    copies = []
    for num, job in enumerate(jobs):
        def keep(place, vals, send=job[4]):
            send[place] = vals.astype(BF)
        product(job, 1, keep)
        copies.append(net.pair_copy(job[4], job[5], send_sem, recv_sem, num))
        copies[-1].start()
        yield
    for copy, job in zip(copies, jobs):
        copy.wait_recv()

        def add(place, vals, out=job[3], recv=job[5]):
            out[place] = (vals + recv[place].astype(F32)).astype(BF)
        product(job, 0, add)
        yield
    for copy in copies:
        copy.wait_send()


def gather_scratch():
    return [pltpu.SemaphoreType.DMA((40,)), pltpu.SemaphoreType.DMA((40,))]


def scatter_scratch(rows, width):
    quarter = rows // 4
    return [pltpu.VMEM((2, 5, 2, 3, quarter, width), BF),
            pltpu.VMEM((2, 5, 2, quarter, width), BF),
            pltpu.VMEM((2, 3, 2 * quarter, width), BF),
            pltpu.VMEM((2, 2 * quarter, width), F32),
            pltpu.SemaphoreType.DMA((60,)), pltpu.SemaphoreType.DMA((60,))]


def vmem_specs(count):
    return [pl.BlockSpec(memory_space=pltpu.VMEM)] * count


def comm_params(ident):
    return pltpu.CompilerParams(collective_id=ident, has_side_effects=True, vmem_limit_bytes=COMM_VMEM[ident])


def normalised(vals):
    mean_val = jnp.mean(vals, axis=-1, keepdims=True)
    centered = vals - mean_val
    var_val = jnp.mean(centered * centered, axis=-1, keepdims=True)
    inv_std = lax.rsqrt(var_val + LN_EPS)
    return centered * inv_std, inv_std


def norm_backward(d_out, vals, gain):
    unit, inv_std = normalised(vals)
    d_unit = d_out * gain
    mean_d = jnp.mean(d_unit, axis=-1, keepdims=True)
    mean_du = jnp.mean(d_unit * unit, axis=-1, keepdims=True)
    d_vals = inv_std * (d_unit - mean_d - unit * mean_du)
    return d_vals, jnp.sum(d_out * unit, axis=0, keepdims=True), jnp.sum(d_out, axis=0, keepdims=True)


def col_sum(vals):
    return jnp.sum(vals, axis=0, keepdims=True)


def first_kernel(group_size, x_ref, par_ref, h_ref, g_send, g_recv):
    net = Net(group_size)
    unit, _ = normalised(x_ref[...].astype(F32))
    h_ref[net.row, net.col] = (unit * par_ref[0:1] + par_ref[1:2]).astype(BF)
    net.barrier()
    for _ in Gather(net, h_ref, g_send, g_recv, x_ref.shape[0]).steps():
        pass


def forward_kernel(group_size, part_ref, res_ref, par_ref, new_ref, h_ref, *scratch):
    net = Net(group_size)
    net.barrier()

    def middle(total):
        new = res_ref[...] + total + par_ref[0:1]
        new_ref[...] = new
        unit, _ = normalised(new)
        h_ref[net.row, net.col] = (unit * par_ref[1:2] + par_ref[2:3]).astype(BF)

    exchanged(net, part_ref, h_ref, scratch, middle, iter(PAIR), BOTH_ORDER)


class SmallSum:
    def __init__(self, net):
        far = range(1, net.side)
        self.net = net
        self.devs = [[net.member(net.row, net.shift(net.col, off)) for off in far], [net.member(net.shift(net.row, off), net.col) for off in far]]

    def barrier(self):
        sem = pltpu.get_barrier_semaphore()
        everyone = self.devs[0] + self.devs[1] + [self.net.partner()]
        for dev in everyone:
            pl.semaphore_signal(sem, inc=1, device_id=dev, device_id_type=MESH)
        pl.semaphore_wait(sem, len(everyone))

    def run(self, in_ref, out_ref, pair_send, pair_recv, buf, sem_s, sem_r):
        net = self.net
        n_half = in_ref.shape[0] // 2
        own, other = [pl.ds(pl.multiple_of(core * n_half, n_half), n_half) for core in (net.core, 1 - net.core)]
        pair_send[...] = in_ref[other].astype(BF)
        copy = net.pair_copy(pair_send, pair_recv, sem_s, sem_r, 0)
        copy.start()
        copy.wait()
        value = in_ref[own] + pair_recv[...].astype(F32)
        for axis in PAIR:
            place = net.row if axis else net.col
            buf[axis, place] = value.astype(BF)
            copies = []
            for num, dev in enumerate(self.devs[axis]):
                ident = 2 + axis * len(self.devs[0]) + num
                copies.append(pltpu.make_async_remote_copy(
                    src_ref=buf.at[axis, place], dst_ref=buf.at[axis, place], send_sem=sem_s.at[ident], recv_sem=sem_r.at[ident],
                    device_id=dev, device_id_type=MESH))
                copies[-1].start()
            for copy in copies:
                copy.wait_recv()
            value = sum(buf[axis, num].astype(F32) for num in range(net.side))
            for copy in copies:
                copy.wait_send()
        out_ref[own] = value
        copy = net.pair_copy(out_ref.at[own], out_ref.at[own], sem_s, sem_r, 1)
        copy.start()
        copy.wait()


def backward_kernel(splits, gathers, group_size, part_ref, res_ref, par_ref, dres_ref, *refs):
    net = Net(group_size)
    small = SmallSum(net)
    if gathers:
        net.barrier(True)
    else:
        small.barrier()
    work, refs = refs[:4], refs[4:]
    if not gathers:
        small_ref, refs = refs[0], refs[1:]
    outs, refs = refs[:2], refs[2:]
    new_ref, sum_ref = refs[:2]
    d_ref = refs[2] if gathers else None
    bufs = refs[3 if gathers else 2:]
    jobs = [(work[2 * num], work[2 * num + 1], split, outs[num], bufs[2 * num], bufs[2 * num + 1]) for num, split in enumerate(splits)]
    send_sem, recv_sem = bufs[4:6]
    bufs = bufs[6:]
    if not gathers:
        stage, small_bufs, bufs = bufs[0], bufs[1:6], bufs[6:]

    def middle(total):
        d_vals, d_gain, d_shift = norm_backward(total, res_ref[...], par_ref[0:1])
        new = dres_ref[...] + d_vals
        new_ref[...] = new.astype(new_ref.dtype)
        if gathers:
            d_ref[net.row, net.col] = new.astype(BF)
            sum_ref[2:3] = col_sum(new)
        else:
            stage[...] = small_ref[...]
        rows = sum_ref if gathers else stage
        rows[0:1] = d_gain
        rows[1:2] = d_shift
        if not gathers:
            small.run(stage, sum_ref, *small_bufs)

    exchanged(net, part_ref, d_ref, bufs, middle, weight_work(net, jobs, send_sem, recv_sem), BOTH_ORDER if gathers else SCATTER_ORDER)


def gelu_tanh(pre_act):
    return jax.nn.gelu(pre_act, approximate=True)


def attention_kernel(group_size, qkv_ref, dy_ref, nat_ref, stat_ref, a_ref, plane_ref, send, score, prob, a_nat, a_part, send_sem, recv_sem, g_send, g_recv):
    net = Net(group_size)
    plane_ref[net.row, net.col] = dy_ref[...]
    net.barrier(True)
    moves = Gather(net, plane_ref, g_send, g_recv, dy_ref.shape[0]).steps()
    parts, n_blk, _, rows, head = nat_ref.shape
    core, n_plane = net.core, n_blk * rows
    for part in range(parts):
        send[part] = qkv_ref[:, (parts + part) * head:(parts + part + 1) * head].reshape(n_blk, rows, head)
    copies = [net.pair_copy(send, nat_ref.at[:, :, core], send_sem, recv_sem, 0)]
    copies[0].start()
    next(moves)
    for part in range(parts):
        nat_ref[part, :, core] = qkv_ref[:, part * head:(part + 1) * head].reshape(n_blk, rows, head)
    copies[0].wait_recv()
    step = n_blk // Q_BLOCKS
    n_q = 2 * step * rows
    factor = head ** -0.5 * LOG2E
    for blk in reversed(range(Q_BLOCKS)):
        here, upto, left = pl.ds(blk * step, step), (blk + 1) * step, blk * n_q
        size = left + n_q
        score[:, :size] = matmul(nat_ref[0, here].reshape(n_q, head), nat_ref[1, :upto].reshape(size, head), NT)

        def softmax_rows(num, carry):
            row = pl.ds(pl.multiple_of(num * ROW_CHUNK, ROW_CHUNK), ROW_CHUNK)
            vals = [score[row, :left]] if left else []
            vals.append(masked(score[row, left:size], num * ROW_CHUNK))
            top = functools.reduce(jnp.maximum, [jnp.max(val, axis=1, keepdims=True) for val in vals])
            exps = [jnp.exp2((val - top) * factor) for val in vals]
            inv = 1.0 / sum(jnp.sum(val, axis=1, keepdims=True) for val in exps)
            if left:
                prob[row, :left] = (exps[0] * inv).astype(BF)
            prob[row, left:size] = (exps[-1] * inv).astype(BF)
            stat = pl.ds(pl.multiple_of(left + num * ROW_CHUNK, ROW_CHUNK), ROW_CHUNK)
            stat_ref[0, stat] = top
            stat_ref[1, stat] = inv
            return carry

        lax.fori_loop(0, n_q // ROW_CHUNK, softmax_rows, 0, unroll=ROW_UNROLL)
        attn = matmul(prob[:, :size], nat_ref[2, :upto].reshape(size, head), NN).astype(BF)
        a_nat[here] = attn.reshape(step, 2, rows, head)
        copies.append(net.pair_copy(a_nat.at[here, 1 - core], a_part.at[here], send_sem, recv_sem, 1 + blk))
        copies[-1].start()
        for _ in range(GATHER_PLAN[Q_BLOCKS - 1 - blk]):
            next(moves, None)
    a_ref[:, :head] = a_nat[:, core].reshape(n_plane, head)
    for copy in copies[1:]:
        copy.wait_recv()
    a_ref[:, head:] = a_part[...].reshape(n_plane, head)
    for _ in moves:
        pass
    for copy in copies:
        copy.wait_send()


def masked(vals, first_row):
    row = first_row + lax.broadcasted_iota(jnp.int32, vals.shape, 0)
    return jnp.where(row >= lax.broadcasted_iota(jnp.int32, vals.shape, 1), vals, -1e30)


def attention_back_kernel(first_row, group_size, d_ref, nat_ref, stat_ref, part_ref, res_ref, bias_ref, dq_ref, y_ref, send, d_nat, score, d_prob, prob, d_score, dk_acc, dv_acc,
                          g_nat, g_part, send_sem, recv_sem, *scratch):
    net = Net(group_size)
    net.barrier(True)
    scatter = Scatter(net, part_ref, *scratch, start=first_row)
    moves = scatter.steps()
    parts, n_blk, _, rows, head = nat_ref.shape
    core, n_plane = net.core, n_blk * rows
    send[...] = d_ref[:, head:].reshape(n_blk, rows, head)
    copies = [net.pair_copy(send, d_nat.at[:, core], send_sem, recv_sem, 0)]
    copies[0].start()
    next(moves)
    d_nat[:, core] = d_ref[:, :head].reshape(n_blk, rows, head)
    copies[0].wait_recv()
    step = n_blk // Q_BLOCKS
    n_q = 2 * step * rows
    scale = head ** -0.5
    for blk in reversed(range(Q_BLOCKS)):
        here, upto, left = pl.ds(blk * step, step), (blk + 1) * step, blk * n_q
        size = left + n_q
        q_vals = nat_ref[0, here].reshape(n_q, head)
        k_vals = nat_ref[1, :upto].reshape(size, head)
        d_vals = d_nat[here].reshape(n_q, head)
        score[:, :size] = matmul(q_vals, k_vals, NT)
        d_prob[:, :size] = matmul(d_vals, nat_ref[2, :upto].reshape(size, head), NT)

        def score_rows(num, carry):
            row = pl.ds(pl.multiple_of(num * BACK_CHUNK, BACK_CHUNK), BACK_CHUNK)
            stat = pl.ds(pl.multiple_of(left + num * BACK_CHUNK, BACK_CHUNK), BACK_CHUNK)
            top, inv = stat_ref[0, stat], stat_ref[1, stat]
            cols = [slice(0, left)] if left else []
            cols.append(slice(left, size))
            probs = []
            for col in cols:
                val = score[row, col]
                if col is cols[-1]:
                    val = masked(val, num * BACK_CHUNK)
                probs.append((jnp.exp2((val - top) * (scale * LOG2E)) * inv).astype(BF))
                prob[row, col] = probs[-1]
            wide = [val.astype(F32) for val in probs]
            grads = [d_prob[row, col] for col in cols]
            dot = sum(jnp.sum(val * grad, axis=1, keepdims=True) for val, grad in zip(wide, grads))
            for col, val, grad in zip(cols, wide, grads):
                d_score[row, col] = (val * (grad - dot) * scale).astype(BF)
            return carry

        lax.fori_loop(0, n_q // BACK_CHUNK, score_rows, 0, unroll=BACK_UNROLL)
        g_nat[0, here] = matmul(d_score[:, :size], k_vals, NN).astype(BF).reshape(step, 2, rows, head)
        for acc, lhs, rhs in ((dk_acc, d_score, q_vals), (dv_acc, prob, d_vals)):
            term = matmul(lhs[:, :size], rhs, TN)
            if blk + 1 == Q_BLOCKS:
                acc[...] = term
            else:
                acc[:size] = acc[:size] + term
        for part, acc in ((1, dk_acc), (2, dv_acc)):
            g_nat[part, here] = acc[left:size].astype(BF).reshape(step, 2, rows, head)
        copies.append(net.pair_copy(g_nat.at[:, here, 1 - core], g_part.at[:, here], send_sem, recv_sem, 1 + blk))
        copies[-1].start()
        next(moves, None)
    for part in range(parts):
        dq_ref[:, part * head:(part + 1) * head] = g_nat[part, :, core].reshape(n_plane, head)
    for copy in copies[1:]:
        copy.wait_recv()
    for part in range(parts):
        dq_ref[:, (parts + part) * head:(parts + part + 1) * head] = g_part[part].reshape(n_plane, head)
    for _ in moves:
        pass
    y_ref[...] = (res_ref[...] + scatter.total() + bias_ref[...]).astype(BF)
    for copy in copies:
        copy.wait_send()


def solution(mesh):
    group_size = mesh.shape['tp']
    side = math.isqrt(group_size // 2)
    if 2 * side * side != group_size or side != len(OFFS):
        raise ValueError('unsupported group')
    swap = [(dev, dev + 1 - 2 * (dev % 2)) for dev in range(group_size)]

    def device_step(x_loc, dy_loc, ln_par, bias_d, w_qkv, w_out, w_up, b_up, w_down):
        n_layers, width = ln_par.shape[0], x_loc.shape[-1]
        rows = x_loc.shape[1]
        n_plane = rows * side * side
        head = w_qkv.shape[-1]
        n_col = w_up.shape[-1]
        plane = jax.ShapeDtypeStruct((side, side, rows, width), BF)
        local_f = jax.ShapeDtypeStruct((rows, width), F32)
        local_b = jax.ShapeDtypeStruct((rows, width), BF)

        def sums(count):
            return jax.ShapeDtypeStruct((count, width), F32)

        def comm(kernel, ident, args, outs, scratch, *static):
            return pl.pallas_call(
                functools.partial(kernel, *static, group_size), name=kernel.__name__, out_shape=outs,
                in_specs=vmem_specs(len(args)), out_specs=jax.tree.map(lambda _: vmem_specs(1)[0], outs),
                scratch_shapes=scratch, compiler_params=comm_params(ident), cost_estimate=COST)(*args)

        block_shape = (side * side, rows, head)
        nat_shape = jax.ShapeDtypeStruct((3, side * side, 2, rows, head), BF)
        n_all, n_q = 2 * n_plane, 2 * n_plane // Q_BLOCKS
        stat_shape = jax.ShapeDtypeStruct((2, n_all, 1), F32)
        pair_sems = [pltpu.SemaphoreType.DMA((1 + Q_BLOCKS,))] * 2

        part_rows = rows // n_layers
        part_scatter = scatter_scratch(part_rows, width)
        one_scatter = scatter_scratch(rows, width)
        both_scratch = one_scatter + gather_scratch()

        def part_slice(layer):
            return slice(layer * part_rows, (layer + 1) * part_rows)

        def swapped(vals):
            return lax.ppermute(vals, 'tp', swap)

        def blocks(part):
            return part.astype(BF).reshape(side, side, rows, width)

        wq_mine = w_qkv.reshape(n_layers, width, 3 * head)
        wq_both = jnp.concatenate([wq_mine, swapped(wq_mine)], axis=2)
        wo_mine = w_out.reshape(n_layers, head, width)
        wo_both = jnp.concatenate([wo_mine, swapped(wo_mine)], axis=1)
        wu_both = jnp.concatenate([w_up, swapped(w_up)], axis=2)
        wd_both = jnp.concatenate([w_down, swapped(w_down)], axis=1)
        bu_both = jnp.concatenate([b_up, swapped(b_up)], axis=1)

        x_rows = x_loc.reshape(rows, width)
        dy_rows = dy_loc.reshape(rows, width)
        h_plane = comm(first_kernel, 0, [x_rows, ln_par[0, 0:2]], plane, gather_scratch())
        res_one = x_rows.astype(F32)
        saved, d_parts, y_parts = [], [], [None] * n_layers
        for layer in range(n_layers):
            h_flat = h_plane.reshape(n_plane, width)
            qkv = matmul(h_flat, wq_both[layer], NN).astype(BF)
            nat, stat, a_both, dy_part = comm(attention_kernel, 6, [qkv, dy_rows[part_slice(layer)]], (
                nat_shape, stat_shape, jax.ShapeDtypeStruct((n_plane, 2 * head), BF), jax.ShapeDtypeStruct((side, side, part_rows, width), BF)), [
                pltpu.VMEM((3,) + block_shape, BF), pltpu.VMEM((n_q, n_all), F32), pltpu.VMEM((n_q, n_all), BF),
                pltpu.VMEM(nat_shape.shape[1:], BF), pltpu.VMEM(block_shape, BF)] + pair_sems + gather_scratch())
            d_parts.append(dy_part)
            part = blocks(matmul(a_both, wo_both[layer], NN))
            par = jnp.concatenate([bias_d[layer, 0:1], ln_par[layer, 2:4]], axis=0)
            res_two, h2_plane = comm(forward_kernel, 1, [part, res_one, par], (local_f, plane), both_scratch)
            h2_flat = h2_plane.reshape(n_plane, width)
            pre_act = matmul(h2_flat, wu_both[layer], NN) + bu_both[layer]
            act_f, gelu_pull = jax.vjp(gelu_tanh, pre_act)
            act = act_f.astype(BF)
            part = blocks(matmul(act, wd_both[layer], NN))
            saved.append((res_one, h_flat, nat, stat, a_both, res_two, h2_flat, gelu_pull, act))
            if layer + 1 < n_layers:
                par = jnp.concatenate([bias_d[layer, 1:2], ln_par[layer + 1, 0:2]], axis=0)
                res_one, h_plane = comm(forward_kernel, 1, [part, res_two, par], (local_f, plane), both_scratch)

        top_part, top_res = part, res_two
        d_plane = jnp.concatenate(d_parts, axis=2)
        def backward(args, splits, shapes, ident, gathers):
            outs = [jax.ShapeDtypeStruct(shape, BF) for shape in shapes]
            outs += [local_f, sums(3), plane] if gathers else [local_b, sums(args[-1].shape[0])]
            bufs = [pltpu.VMEM(shape, BF) for shape in shapes for _ in PAIR] + [pltpu.SemaphoreType.DMA((2,))] * 2
            if not gathers:
                count = args[-1].shape[0]
                half = (count // 2, width)
                bufs += [pltpu.VMEM((count, width), F32), pltpu.VMEM(half, BF), pltpu.VMEM(half, BF), pltpu.VMEM((2, side) + half, BF)]
                bufs += [pltpu.SemaphoreType.DMA((2 * side,))] * 2
            return comm(backward_kernel, ident, args, tuple(outs), bufs + one_scatter + gather_scratch() * gathers, splits, gathers)

        d_res = dy_rows.astype(F32)
        bias_two = jnp.sum(d_res, axis=0, keepdims=True)
        grads, smalls = [None] * n_layers, []
        for layer in reversed(range(n_layers)):
            res_one, h_flat, nat, stat, a_both, res_two, h2_flat, gelu_pull, act = saved[layer]
            d_flat = d_plane.reshape(n_plane, width)
            d_act = matmul(d_flat, wd_both[layer], NT)
            d_pre = gelu_pull(d_act)[0]
            d_pre_bf = d_pre.astype(BF)
            d_bup = jnp.sum(d_pre, axis=0)
            part = blocks(matmul(d_pre_bf, wu_both[layer], NT))
            d_wdown, d_wup, d_res, sum_two, da_plane = backward(
                [part, res_two, ln_par[layer, 2:3], d_res, act, d_flat, h2_flat, d_pre_bf], (True, False),
                [(n_col, width), (width, n_col)], 3, True)
            da_flat = da_plane.reshape(n_plane, width)
            d_both = matmul(da_flat, wo_both[layer], NT).astype(BF)
            dq_both, y_part = comm(attention_back_kernel, 7 + layer, [d_both, nat, stat, top_part, top_res[part_slice(layer)], bias_d[n_layers - 1, 1:2]], (
                jax.ShapeDtypeStruct((n_plane, 6 * head), BF), jax.ShapeDtypeStruct((part_rows, width), BF)), [
                pltpu.VMEM(block_shape, BF), pltpu.VMEM(nat_shape.shape[1:], BF), pltpu.VMEM((n_q, n_all), F32),
                pltpu.VMEM((n_q, n_all), F32), pltpu.VMEM((n_q, n_all), BF), pltpu.VMEM((n_q, n_all), BF),
                pltpu.VMEM((n_all, head), F32), pltpu.VMEM((n_all, head), F32), pltpu.VMEM(nat_shape.shape, BF),
                pltpu.VMEM((3,) + block_shape, BF)] + pair_sems + part_scatter, layer * part_rows)
            y_parts[layer] = y_part
            part = blocks(matmul(dq_both, wq_both[layer], NT))
            args = [part, res_one, ln_par[layer, 0:1], d_res, a_both, da_flat, h_flat, dq_both]
            shapes = [(head, width), (width, 3 * head)]
            others = [sum_two[0:2], sum_two[2:3], bias_two]
            if layer > 0:
                d_wout, d_wqkv, d_res, sum_one, d_plane = backward(args, (True, False), shapes, 4, True)
                bias_two = sum_one[2:3]
                smalls = [sum_one[0:2]] + others + smalls
            else:
                smalls = [jnp.zeros((2, width), F32)] + others + smalls
                n_small = sum(piece.shape[0] for piece in smalls)
                packed = jnp.concatenate(smalls + [jnp.zeros((-n_small % 16, width), F32)], axis=0)
                d_wout, d_wqkv, x_grad, total = backward(args + [packed], (True, False), shapes, 5, False)
            grads[layer] = (d_wqkv, d_wout, d_wup, d_bup[:n_col] + swapped(d_bup[n_col:]), d_wdown)
        total = total[:n_small].reshape(n_layers, n_small // n_layers, width)
        return (jnp.concatenate(y_parts, axis=0).reshape(x_loc.shape), x_grad.reshape(x_loc.shape), total[:, :4], total[:, 4:],
                jnp.stack([grad[0].reshape(width, 3, 1, head) for grad in grads]),
                jnp.stack([grad[1].reshape(1, head, width) for grad in grads]),
                jnp.stack([grad[2] for grad in grads]),
                jnp.stack([grad[3] for grad in grads]),
                jnp.stack([grad[4] for grad in grads]))

    def on_tp(dim, first=None):
        return P(first, *[None] * (dim - 1), 'tp')

    rows_spec = P('dp', 'tp')
    in_specs = (rows_spec, rows_spec, P(), P(), on_tp(3), on_tp(1), on_tp(2), on_tp(1), on_tp(1))
    out_specs = (rows_spec, rows_spec, P('dp'), P('dp'), on_tp(3, 'dp'), on_tp(1, 'dp'), on_tp(2, 'dp'), on_tp(1, 'dp'), on_tp(1, 'dp'))
    return jax.shard_map(device_step, mesh=mesh, in_specs=in_specs, out_specs=out_specs, check_vma=False)
```

```python
import functools
import math

import jax
import jax.numpy as jnp
from jax import lax
from jax.experimental import pallas as pl
from jax.experimental.pallas import tpu as pltpu
from jax.sharding import PartitionSpec as P

MESH = pl.DeviceIdType.MESH
BF = jnp.bfloat16
F32 = jnp.float32
LN_EPS = 1e-5
OFFS = (0, -1, 1, 2)
RS_ORDER = (2, 1, -1, 0)
PAIR = (0, 1)
WAYS = (1, -1)
LATE = (2, 3)
NN = ((1,), (0,))
NT = ((1,), (1,))
TN = ((0,), (0,))
MIB = 1 << 20
COMM_VMEM = [size * MIB for size in (4, 10, 6, 16, 14, 14, 12, 20, 20)]
Q_BLOCKS = 8
ROW_CHUNK = 64
BACK_CHUNK = 64
ROW_UNROLL = 4
BACK_UNROLL = 2
LOG2E = math.log2(math.e)
BOTH_ORDER = 'axaaaxaaaaaamccdxccxcccc'
SCATTER_ORDER = 'axaxaaxaaxaaamd'
WORK_CHUNK = 512
COST = pl.CostEstimate(flops=20 * 10 ** 9, bytes_accessed=MIB, transcendentals=0)
GATHER_PLAN = [int(code) for code in '01011111']


def matmul(lhs, rhs, dims):
    return lax.dot_general(lhs, rhs, (dims, ((), ())), preferred_element_type=F32)


class Net:
    def __init__(self, group_size):
        side = math.isqrt(group_size // 2)
        me = lax.axis_index('tp')
        self.side = side
        self.core = lax.rem(me, 2)
        self.col = lax.rem(me // 2, side)
        self.row = me // (2 * side)

    def shift(self, pos, off):
        return lax.rem(pos + (off + self.side), self.side)

    def block(self, half, first, second):
        if half == 0:
            return self.shift(self.row, second), self.shift(self.col, first)
        return self.shift(self.row, first), self.shift(self.col, second)

    def neighbour(self, half, axis, sgn):
        if (axis == 0) == (half == 0):
            row, col = self.row, self.shift(self.col, sgn)
        else:
            row, col = self.shift(self.row, sgn), self.col
        return self.member(row, col)

    def member(self, row, col):
        return {'tp': (row * self.side + col) * 2 + self.core}

    def partner(self):
        return {'tp': (self.row * self.side + self.col) * 2 + (1 - self.core)}

    def pair_copy(self, src, dst, send_sem, recv_sem, num):
        return pltpu.make_async_remote_copy(src_ref=src, dst_ref=dst, send_sem=send_sem.at[num], recv_sem=recv_sem.at[num],
                                            device_id=self.partner(), device_id_type=MESH)

    def barrier(self, with_partner=False):
        sem = pltpu.get_barrier_semaphore()
        targets = [self.neighbour(half, 0, sgn) for half in PAIR for sgn in WAYS] + [self.partner()] * with_partner
        for target in targets:
            pl.semaphore_signal(sem, inc=1, device_id=target, device_id_type=MESH)
        pl.semaphore_wait(sem, len(targets))


class Gather:
    def __init__(self, net, buf, send_sem, recv_sem, rows, start=0):
        self.net, self.buf, self.send_sem, self.recv_sem = net, buf, send_sem, recv_sem
        self.rows, self.base = rows, start
        self.sent = []

    def ident(self, half, stage, first, kind):
        return half * 20 + (0 if stage == 0 else 4 + 4 * OFFS.index(first)) + kind

    def slot(self, half, first, second, kind):
        row, col = self.net.block(half, first, second)
        n_half = self.rows // 2
        start, size = self.base + half * n_half, n_half
        if kind >= 2:
            size = n_half // 2
            start += (kind - 2) * size
        return self.buf.at[row, col, pl.ds(start, size)]

    def copy(self, half, stage, first, kind, ref):
        ident = self.ident(half, stage, first, kind)
        sgn = 1 if kind % 2 == 0 else -1
        return pltpu.make_async_remote_copy(
            src_ref=ref, dst_ref=ref, send_sem=self.send_sem.at[ident], recv_sem=self.recv_sem.at[ident],
            device_id=self.net.neighbour(half, stage, sgn), device_id_type=MESH)

    def send(self, half, stage, first, kind):
        back = (0, 0, -1, 1)[kind]
        offs = (back, 0) if stage == 0 else (first, back)
        copy = self.copy(half, stage, first, kind, self.slot(half, offs[0], offs[1], kind))
        copy.start()
        self.sent.append(copy)

    def wait(self, half, stage, first, kind):
        back = (-1, 1, 2, 2)[kind]
        offs = (back, 0) if stage == 0 else (first, back)
        self.copy(half, stage, first, kind, self.slot(half, offs[0], offs[1], kind)).wait_recv()

    def each(self, call, stage, first, kinds):
        for kind in kinds:
            for half in PAIR:
                call(half, stage, first, kind)

    def onward(self, half, stage, first, kind):
        self.wait(half, stage, first, kind)
        self.send(half, stage, first, kind + 2)

    def steps(self):
        self.each(self.send, 0, 0, PAIR)
        self.each(self.send, 1, 0, PAIR)
        yield
        for kind in PAIR:
            for half in PAIR:
                self.onward(half, 0, 0, kind)
                for way in PAIR:
                    self.send(half, 1, -WAYS[kind], way)
        yield
        self.each(self.onward, 1, 0, PAIR)
        yield
        self.each(self.wait, 0, 0, LATE)
        self.each(self.send, 1, 2, PAIR)
        yield
        for first in OFFS[1:]:
            self.each(self.onward, 1, first, PAIR)
            yield
        for first in OFFS:
            self.each(self.wait, 1, first, LATE)
        for copy in self.sent:
            copy.wait_send()


class Scatter:
    def __init__(self, net, part, recv, out, held, last, send_sem, recv_sem, start=0):
        self.net, self.part, self.recv, self.out, self.held, self.last = net, part, recv, out, held, last
        self.send_sem, self.recv_sem = send_sem, recv_sem
        self.quarter, self.base = recv.shape[-2], start
        self.sent = []

    def copy(self, half, stage, way, kind, ref):
        ident = ((half * 5 + stage) * 2 + way) * 3 + kind
        return pltpu.make_async_remote_copy(
            src_ref=ref, dst_ref=self.recv.at[half, stage, way, kind],
            send_sem=self.send_sem.at[ident], recv_sem=self.recv_sem.at[ident],
            device_id=self.net.neighbour(half, 0 if stage == 4 else 1, WAYS[way]), device_id_type=MESH)

    def send(self, half, stage, way, kind, ref):
        copy = self.copy(half, stage, way, kind, ref)
        copy.start()
        self.sent.append(copy)

    def wait(self, half, stage, way, kind):
        self.copy(half, stage, way, kind, self.recv.at[half, stage, way, kind]).wait_recv()

    def term(self, half, stage, off, sub):
        if stage == 4:
            return self.held.at[half, {2: 0, 1: 1, -1: 2}[off], pl.ds(sub * self.quarter, self.quarter)]
        row, col = self.net.block(half, RS_ORDER[stage], off)
        return self.part.at[row, col, pl.ds(self.base + (2 * half + sub) * self.quarter, self.quarter)]

    def far(self, half, stage):
        for way in PAIR:
            self.send(half, stage, way, 0, self.term(half, stage, 2, way))

    def near_plain(self, half, stage, way):
        self.send(half, stage, way, 1, self.term(half, stage, WAYS[way], 1 - way))

    def near_summed(self, half, stage, way):
        self.wait(half, stage, way, 0)
        total = self.term(half, stage, WAYS[way], way)[...].astype(F32) + self.recv[half, stage, way, 0].astype(F32)
        self.out[half, stage, way] = total.astype(BF)
        self.send(half, stage, way, 2, self.out.at[half, stage, way])

    def arrived(self, half, stage, sub):
        first = self.recv[half, stage, 0, 2 if sub == 0 else 1].astype(F32)
        second = self.recv[half, stage, 1, 1 if sub == 0 else 2].astype(F32)
        return first + second

    def finish(self, half, stage):
        for way in PAIR:
            self.wait(half, stage, way, 1)
            self.wait(half, stage, way, 2)
        for sub in PAIR:
            total = self.term(half, stage, 0, sub)[...].astype(F32) + self.arrived(half, stage, sub)
            rows = pl.ds(sub * self.quarter, self.quarter)
            if stage < 3:
                self.held[half, stage, rows] = total.astype(BF)
            else:
                self.last[half, rows] = total

    def near(self, stage):
        for half in PAIR:
            for way in PAIR:
                self.near_summed(half, stage, way)
                self.near_plain(half, stage, way)

    def steps(self):
        last = len(OFFS)
        for stage in range(last):
            for half in PAIR:
                self.far(half, stage)
        yield
        for stage in range(last - 1):
            self.near(stage)
            yield
        for half in PAIR:
            self.finish(half, 0)
            self.far(half, last)
        yield
        self.near(last - 1)
        yield
        for stage in (1, 2):
            for half in PAIR:
                self.finish(half, stage)
                self.near_plain(half, last, stage - 1)
        yield
        for half in PAIR:
            for way in PAIR:
                self.near_summed(half, last, way)
        yield
        for half in PAIR:
            self.finish(half, last - 1)
        yield
        for half in PAIR:
            for way in PAIR:
                self.wait(half, last, way, 1)
                self.wait(half, last, way, 2)
            for sub in PAIR:
                rows = pl.ds(sub * self.quarter, self.quarter)
                self.last[half, rows] = self.last[half, rows] + self.arrived(half, last, sub)

    def drain(self):
        for copy in self.sent:
            copy.wait_send()

    def total(self):
        n_half, width = self.last.shape[1:]
        return self.last[...].reshape(2 * n_half, width)


def exchanged(net, part_ref, out_ref, scratch, middle, other, order):
    scatter = Scatter(net, part_ref, *scratch[:6])
    tasks = {'a': scatter.steps(), 'x': other}
    if out_ref is not None:
        tasks['c'] = Gather(net, out_ref, *scratch[6:], part_ref.shape[2]).steps()
    for code in order:
        if code == 'm':
            for _ in tasks['a']:
                pass
            middle(scatter.total())
        elif code == 'd':
            scatter.drain()
        else:
            next(tasks[code], None)
    for task in tasks.values():
        for _ in task:
            pass


def weight_work(net, jobs, send_sem, recv_sem):
    def product(job, which, store):
        left, right, split_left, out = job[:4]
        count = out.shape[0] if split_left else out.shape[1]
        own = slice(which * count, (which + 1) * count)
        wide = right.shape[1] if split_left else left.shape[1]

        def chunk(num, carry):
            cols = pl.ds(pl.multiple_of(num * WORK_CHUNK, WORK_CHUNK), WORK_CHUNK)
            if split_left:
                store((slice(None), cols), matmul(left[:, own], right[:, cols], TN))
            else:
                store((cols, slice(None)), matmul(left[:, cols], right[:, own], TN))
            return carry

        lax.fori_loop(0, wide // WORK_CHUNK, chunk, 0)

    copies = []
    for num, job in enumerate(jobs):
        def keep(place, vals, send=job[4]):
            send[place] = vals.astype(BF)
        product(job, 1, keep)
        copies.append(net.pair_copy(job[4], job[5], send_sem, recv_sem, num))
        copies[-1].start()
        yield
    for copy, job in zip(copies, jobs):
        copy.wait_recv()

        def add(place, vals, out=job[3], recv=job[5]):
            out[place] = (vals + recv[place].astype(F32)).astype(BF)
        product(job, 0, add)
        yield
    for copy in copies:
        copy.wait_send()


def gather_scratch():
    return [pltpu.SemaphoreType.DMA((40,)), pltpu.SemaphoreType.DMA((40,))]


def scatter_scratch(rows, width):
    quarter = rows // 4
    return [pltpu.VMEM((2, 5, 2, 3, quarter, width), BF),
            pltpu.VMEM((2, 5, 2, quarter, width), BF),
            pltpu.VMEM((2, 3, 2 * quarter, width), BF),
            pltpu.VMEM((2, 2 * quarter, width), F32),
            pltpu.SemaphoreType.DMA((60,)), pltpu.SemaphoreType.DMA((60,))]


def vmem_specs(count):
    return [pl.BlockSpec(memory_space=pltpu.VMEM)] * count


def comm_params(ident):
    return pltpu.CompilerParams(collective_id=ident, has_side_effects=True, vmem_limit_bytes=COMM_VMEM[ident])


def normalised(vals):
    mean_val = jnp.mean(vals, axis=-1, keepdims=True)
    centered = vals - mean_val
    var_val = jnp.mean(centered * centered, axis=-1, keepdims=True)
    inv_std = lax.rsqrt(var_val + LN_EPS)
    return centered * inv_std, inv_std


def norm_backward(d_out, vals, gain):
    unit, inv_std = normalised(vals)
    d_unit = d_out * gain
    mean_d = jnp.mean(d_unit, axis=-1, keepdims=True)
    mean_du = jnp.mean(d_unit * unit, axis=-1, keepdims=True)
    d_vals = inv_std * (d_unit - mean_d - unit * mean_du)
    return d_vals, jnp.sum(d_out * unit, axis=0, keepdims=True), jnp.sum(d_out, axis=0, keepdims=True)


def col_sum(vals):
    return jnp.sum(vals, axis=0, keepdims=True)


def first_kernel(group_size, x_ref, par_ref, h_ref, g_send, g_recv):
    net = Net(group_size)
    unit, _ = normalised(x_ref[...].astype(F32))
    h_ref[net.row, net.col] = (unit * par_ref[0:1] + par_ref[1:2]).astype(BF)
    net.barrier()
    for _ in Gather(net, h_ref, g_send, g_recv, x_ref.shape[0]).steps():
        pass


def forward_kernel(group_size, part_ref, res_ref, par_ref, new_ref, h_ref, *scratch):
    net = Net(group_size)
    net.barrier()

    def middle(total):
        new = res_ref[...] + total + par_ref[0:1]
        new_ref[...] = new
        unit, _ = normalised(new)
        h_ref[net.row, net.col] = (unit * par_ref[1:2] + par_ref[2:3]).astype(BF)

    exchanged(net, part_ref, h_ref, scratch, middle, iter(PAIR), BOTH_ORDER)


class SmallSum:
    def __init__(self, net):
        far = range(1, net.side)
        self.net = net
        self.devs = [[net.member(net.row, net.shift(net.col, off)) for off in far], [net.member(net.shift(net.row, off), net.col) for off in far]]

    def barrier(self):
        sem = pltpu.get_barrier_semaphore()
        everyone = self.devs[0] + self.devs[1] + [self.net.partner()]
        for dev in everyone:
            pl.semaphore_signal(sem, inc=1, device_id=dev, device_id_type=MESH)
        pl.semaphore_wait(sem, len(everyone))

    def run(self, in_ref, out_ref, pair_send, pair_recv, buf, sem_s, sem_r):
        net = self.net
        n_half = in_ref.shape[0] // 2
        own, other = [pl.ds(pl.multiple_of(core * n_half, n_half), n_half) for core in (net.core, 1 - net.core)]
        pair_send[...] = in_ref[other].astype(BF)
        copy = net.pair_copy(pair_send, pair_recv, sem_s, sem_r, 0)
        copy.start()
        copy.wait()
        value = in_ref[own] + pair_recv[...].astype(F32)
        for axis in PAIR:
            place = net.row if axis else net.col
            buf[axis, place] = value.astype(BF)
            copies = []
            for num, dev in enumerate(self.devs[axis]):
                ident = 2 + axis * len(self.devs[0]) + num
                copies.append(pltpu.make_async_remote_copy(
                    src_ref=buf.at[axis, place], dst_ref=buf.at[axis, place], send_sem=sem_s.at[ident], recv_sem=sem_r.at[ident],
                    device_id=dev, device_id_type=MESH))
                copies[-1].start()
            for copy in copies:
                copy.wait_recv()
            value = sum(buf[axis, num].astype(F32) for num in range(net.side))
            for copy in copies:
                copy.wait_send()
        out_ref[own] = value
        copy = net.pair_copy(out_ref.at[own], out_ref.at[own], sem_s, sem_r, 1)
        copy.start()
        copy.wait()


def backward_kernel(splits, gathers, group_size, part_ref, res_ref, par_ref, dres_ref, *refs):
    net = Net(group_size)
    small = SmallSum(net)
    if gathers:
        net.barrier(True)
    else:
        small.barrier()
    work, refs = refs[:4], refs[4:]
    if not gathers:
        small_ref, refs = refs[0], refs[1:]
    outs, refs = refs[:2], refs[2:]
    new_ref, sum_ref = refs[:2]
    d_ref = refs[2] if gathers else None
    bufs = refs[3 if gathers else 2:]
    jobs = [(work[2 * num], work[2 * num + 1], split, outs[num], bufs[2 * num], bufs[2 * num + 1]) for num, split in enumerate(splits)]
    send_sem, recv_sem = bufs[4:6]
    bufs = bufs[6:]
    if not gathers:
        stage, small_bufs, bufs = bufs[0], bufs[1:6], bufs[6:]

    def middle(total):
        d_vals, d_gain, d_shift = norm_backward(total, res_ref[...], par_ref[0:1])
        new = dres_ref[...] + d_vals
        new_ref[...] = new.astype(new_ref.dtype)
        if gathers:
            d_ref[net.row, net.col] = new.astype(BF)
            sum_ref[2:3] = col_sum(new)
        else:
            stage[...] = small_ref[...]
        rows = sum_ref if gathers else stage
        rows[0:1] = d_gain
        rows[1:2] = d_shift
        if not gathers:
            small.run(stage, sum_ref, *small_bufs)

    exchanged(net, part_ref, d_ref, bufs, middle, weight_work(net, jobs, send_sem, recv_sem), BOTH_ORDER if gathers else SCATTER_ORDER)


def gelu_tanh(pre_act):
    return jax.nn.gelu(pre_act, approximate=True)


def attention_kernel(group_size, qkv_ref, dy_ref, nat_ref, stat_ref, a_ref, plane_ref, send, score, prob, a_nat, a_part, send_sem, recv_sem, g_send, g_recv):
    net = Net(group_size)
    plane_ref[net.row, net.col] = dy_ref[...]
    net.barrier(True)
    moves = Gather(net, plane_ref, g_send, g_recv, dy_ref.shape[0]).steps()
    parts, n_blk, _, rows, head = nat_ref.shape
    core, n_plane = net.core, n_blk * rows
    for part in range(parts):
        send[part] = qkv_ref[:, (parts + part) * head:(parts + part + 1) * head].reshape(n_blk, rows, head)
    copies = [net.pair_copy(send, nat_ref.at[:, :, core], send_sem, recv_sem, 0)]
    copies[0].start()
    next(moves)
    for part in range(parts):
        nat_ref[part, :, core] = qkv_ref[:, part * head:(part + 1) * head].reshape(n_blk, rows, head)
    copies[0].wait_recv()
    step = n_blk // Q_BLOCKS
    n_q = 2 * step * rows
    factor = head ** -0.5 * LOG2E
    for blk in reversed(range(Q_BLOCKS)):
        here, upto, left = pl.ds(blk * step, step), (blk + 1) * step, blk * n_q
        size = left + n_q
        score[:, :size] = matmul(nat_ref[0, here].reshape(n_q, head), nat_ref[1, :upto].reshape(size, head), NT)

        def softmax_rows(num, carry):
            row = pl.ds(pl.multiple_of(num * ROW_CHUNK, ROW_CHUNK), ROW_CHUNK)
            vals = [score[row, :left]] if left else []
            vals.append(masked(score[row, left:size], num * ROW_CHUNK))
            top = functools.reduce(jnp.maximum, [jnp.max(val, axis=1, keepdims=True) for val in vals])
            exps = [jnp.exp2((val - top) * factor) for val in vals]
            inv = 1.0 / sum(jnp.sum(val, axis=1, keepdims=True) for val in exps)
            if left:
                prob[row, :left] = (exps[0] * inv).astype(BF)
            prob[row, left:size] = (exps[-1] * inv).astype(BF)
            stat = pl.ds(pl.multiple_of(left + num * ROW_CHUNK, ROW_CHUNK), ROW_CHUNK)
            stat_ref[0, stat] = top
            stat_ref[1, stat] = inv
            return carry

        lax.fori_loop(0, n_q // ROW_CHUNK, softmax_rows, 0, unroll=ROW_UNROLL)
        attn = matmul(prob[:, :size], nat_ref[2, :upto].reshape(size, head), NN).astype(BF)
        a_nat[here] = attn.reshape(step, 2, rows, head)
        copies.append(net.pair_copy(a_nat.at[here, 1 - core], a_part.at[here], send_sem, recv_sem, 1 + blk))
        copies[-1].start()
        for _ in range(GATHER_PLAN[Q_BLOCKS - 1 - blk]):
            next(moves, None)
    a_ref[:, :head] = a_nat[:, core].reshape(n_plane, head)
    for copy in copies[1:]:
        copy.wait_recv()
    a_ref[:, head:] = a_part[...].reshape(n_plane, head)
    for _ in moves:
        pass
    for copy in copies:
        copy.wait_send()


def masked(vals, first_row):
    row = first_row + lax.broadcasted_iota(jnp.int32, vals.shape, 0)
    return jnp.where(row >= lax.broadcasted_iota(jnp.int32, vals.shape, 1), vals, -1e30)


def attention_back_kernel(first_row, group_size, d_ref, nat_ref, stat_ref, part_ref, res_ref, bias_ref, dq_ref, y_ref, send, d_nat, score, d_prob, prob, d_score, dk_acc, dv_acc,
                          g_nat, g_part, send_sem, recv_sem, *scratch):
    net = Net(group_size)
    net.barrier(True)
    scatter = Scatter(net, part_ref, *scratch, start=first_row)
    moves = scatter.steps()
    parts, n_blk, _, rows, head = nat_ref.shape
    core, n_plane = net.core, n_blk * rows
    send[...] = d_ref[:, head:].reshape(n_blk, rows, head)
    copies = [net.pair_copy(send, d_nat.at[:, core], send_sem, recv_sem, 0)]
    copies[0].start()
    next(moves)
    d_nat[:, core] = d_ref[:, :head].reshape(n_blk, rows, head)
    copies[0].wait_recv()
    step = n_blk // Q_BLOCKS
    n_q = 2 * step * rows
    scale = head ** -0.5
    for blk in reversed(range(Q_BLOCKS)):
        here, upto, left = pl.ds(blk * step, step), (blk + 1) * step, blk * n_q
        size = left + n_q
        q_vals = nat_ref[0, here].reshape(n_q, head)
        k_vals = nat_ref[1, :upto].reshape(size, head)
        d_vals = d_nat[here].reshape(n_q, head)
        score[:, :size] = matmul(q_vals, k_vals, NT)
        d_prob[:, :size] = matmul(d_vals, nat_ref[2, :upto].reshape(size, head), NT)

        def score_rows(num, carry):
            row = pl.ds(pl.multiple_of(num * BACK_CHUNK, BACK_CHUNK), BACK_CHUNK)
            stat = pl.ds(pl.multiple_of(left + num * BACK_CHUNK, BACK_CHUNK), BACK_CHUNK)
            top, inv = stat_ref[0, stat], stat_ref[1, stat]
            cols = [slice(0, left)] if left else []
            cols.append(slice(left, size))
            probs = []
            for col in cols:
                val = score[row, col]
                if col is cols[-1]:
                    val = masked(val, num * BACK_CHUNK)
                probs.append((jnp.exp2((val - top) * (scale * LOG2E)) * inv).astype(BF))
                prob[row, col] = probs[-1]
            wide = [val.astype(F32) for val in probs]
            grads = [d_prob[row, col] for col in cols]
            dot = sum(jnp.sum(val * grad, axis=1, keepdims=True) for val, grad in zip(wide, grads))
            for col, val, grad in zip(cols, wide, grads):
                d_score[row, col] = (val * (grad - dot) * scale).astype(BF)
            return carry

        lax.fori_loop(0, n_q // BACK_CHUNK, score_rows, 0, unroll=BACK_UNROLL)
        g_nat[0, here] = matmul(d_score[:, :size], k_vals, NN).astype(BF).reshape(step, 2, rows, head)
        for acc, lhs, rhs in ((dk_acc, d_score, q_vals), (dv_acc, prob, d_vals)):
            term = matmul(lhs[:, :size], rhs, TN)
            if blk + 1 == Q_BLOCKS:
                acc[...] = term
            else:
                acc[:size] = acc[:size] + term
        for part, acc in ((1, dk_acc), (2, dv_acc)):
            g_nat[part, here] = acc[left:size].astype(BF).reshape(step, 2, rows, head)
        copies.append(net.pair_copy(g_nat.at[:, here, 1 - core], g_part.at[:, here], send_sem, recv_sem, 1 + blk))
        copies[-1].start()
        next(moves, None)
    for part in range(parts):
        dq_ref[:, part * head:(part + 1) * head] = g_nat[part, :, core].reshape(n_plane, head)
    for copy in copies[1:]:
        copy.wait_recv()
    for part in range(parts):
        dq_ref[:, (parts + part) * head:(parts + part + 1) * head] = g_part[part].reshape(n_plane, head)
    for _ in moves:
        pass
    scatter.drain()
    y_ref[...] = (res_ref[...] + scatter.total() + bias_ref[...]).astype(BF)
    for copy in copies:
        copy.wait_send()


def solution(mesh):
    group_size = mesh.shape['tp']
    side = math.isqrt(group_size // 2)
    if 2 * side * side != group_size or side != len(OFFS):
        raise ValueError('unsupported group')
    swap = [(dev, dev + 1 - 2 * (dev % 2)) for dev in range(group_size)]

    def device_step(x_loc, dy_loc, ln_par, bias_d, w_qkv, w_out, w_up, b_up, w_down):
        n_layers, width = ln_par.shape[0], x_loc.shape[-1]
        rows = x_loc.shape[1]
        n_plane = rows * side * side
        head = w_qkv.shape[-1]
        n_col = w_up.shape[-1]
        plane = jax.ShapeDtypeStruct((side, side, rows, width), BF)
        local_f = jax.ShapeDtypeStruct((rows, width), F32)
        local_b = jax.ShapeDtypeStruct((rows, width), BF)

        def sums(count):
            return jax.ShapeDtypeStruct((count, width), F32)

        def comm(kernel, ident, args, outs, scratch, *static):
            return pl.pallas_call(
                functools.partial(kernel, *static, group_size), name=kernel.__name__, out_shape=outs,
                in_specs=vmem_specs(len(args)), out_specs=jax.tree.map(lambda _: vmem_specs(1)[0], outs),
                scratch_shapes=scratch, compiler_params=comm_params(ident), cost_estimate=COST)(*args)

        block_shape = (side * side, rows, head)
        nat_shape = jax.ShapeDtypeStruct((3, side * side, 2, rows, head), BF)
        n_all, n_q = 2 * n_plane, 2 * n_plane // Q_BLOCKS
        stat_shape = jax.ShapeDtypeStruct((2, n_all, 1), F32)
        pair_sems = [pltpu.SemaphoreType.DMA((1 + Q_BLOCKS,))] * 2

        part_rows = rows // n_layers
        part_scatter = scatter_scratch(part_rows, width)
        one_scatter = scatter_scratch(rows, width)
        both_scratch = one_scatter + gather_scratch()

        def part_slice(layer):
            return slice(layer * part_rows, (layer + 1) * part_rows)

        def swapped(vals):
            return lax.ppermute(vals, 'tp', swap)

        def blocks(part):
            return part.astype(BF).reshape(side, side, rows, width)

        wq_mine = w_qkv.reshape(n_layers, width, 3 * head)
        wq_both = jnp.concatenate([wq_mine, swapped(wq_mine)], axis=2)
        wo_mine = w_out.reshape(n_layers, head, width)
        wo_both = jnp.concatenate([wo_mine, swapped(wo_mine)], axis=1)
        wu_both = jnp.concatenate([w_up, swapped(w_up)], axis=2)
        wd_both = jnp.concatenate([w_down, swapped(w_down)], axis=1)
        bu_both = jnp.concatenate([b_up, swapped(b_up)], axis=1)

        x_rows = x_loc.reshape(rows, width)
        dy_rows = dy_loc.reshape(rows, width)
        h_plane = comm(first_kernel, 0, [x_rows, ln_par[0, 0:2]], plane, gather_scratch())
        res_one = x_rows.astype(F32)
        saved, d_parts, y_parts = [], [], [None] * n_layers
        for layer in range(n_layers):
            h_flat = h_plane.reshape(n_plane, width)
            qkv = matmul(h_flat, wq_both[layer], NN).astype(BF)
            nat, stat, a_both, dy_part = comm(attention_kernel, 6, [qkv, dy_rows[part_slice(layer)]], (
                nat_shape, stat_shape, jax.ShapeDtypeStruct((n_plane, 2 * head), BF), jax.ShapeDtypeStruct((side, side, part_rows, width), BF)), [
                pltpu.VMEM((3,) + block_shape, BF), pltpu.VMEM((n_q, n_all), F32), pltpu.VMEM((n_q, n_all), BF),
                pltpu.VMEM(nat_shape.shape[1:], BF), pltpu.VMEM(block_shape, BF)] + pair_sems + gather_scratch())
            d_parts.append(dy_part)
            part = blocks(matmul(a_both, wo_both[layer], NN))
            par = jnp.concatenate([bias_d[layer, 0:1], ln_par[layer, 2:4]], axis=0)
            res_two, h2_plane = comm(forward_kernel, 1, [part, res_one, par], (local_f, plane), both_scratch)
            h2_flat = h2_plane.reshape(n_plane, width)
            pre_act = matmul(h2_flat, wu_both[layer], NN) + bu_both[layer]
            act_f, gelu_pull = jax.vjp(gelu_tanh, pre_act)
            act = act_f.astype(BF)
            part = blocks(matmul(act, wd_both[layer], NN))
            saved.append((res_one, h_flat, nat, stat, a_both, res_two, h2_flat, gelu_pull, act))
            if layer + 1 < n_layers:
                par = jnp.concatenate([bias_d[layer, 1:2], ln_par[layer + 1, 0:2]], axis=0)
                res_one, h_plane = comm(forward_kernel, 1, [part, res_two, par], (local_f, plane), both_scratch)

        top_part, top_res = part, res_two
        d_plane = jnp.concatenate(d_parts, axis=2)
        def backward(args, splits, shapes, ident, gathers):
            outs = [jax.ShapeDtypeStruct(shape, BF) for shape in shapes]
            outs += [local_f, sums(3), plane] if gathers else [local_b, sums(args[-1].shape[0])]
            bufs = [pltpu.VMEM(shape, BF) for shape in shapes for _ in PAIR] + [pltpu.SemaphoreType.DMA((2,))] * 2
            if not gathers:
                count = args[-1].shape[0]
                half = (count // 2, width)
                bufs += [pltpu.VMEM((count, width), F32), pltpu.VMEM(half, BF), pltpu.VMEM(half, BF), pltpu.VMEM((2, side) + half, BF)]
                bufs += [pltpu.SemaphoreType.DMA((2 * side,))] * 2
            return comm(backward_kernel, ident, args, tuple(outs), bufs + one_scatter + gather_scratch() * gathers, splits, gathers)

        d_res = dy_rows.astype(F32)
        bias_two = jnp.sum(d_res, axis=0, keepdims=True)
        grads, smalls = [None] * n_layers, []
        for layer in reversed(range(n_layers)):
            res_one, h_flat, nat, stat, a_both, res_two, h2_flat, gelu_pull, act = saved[layer]
            d_flat = d_plane.reshape(n_plane, width)
            d_act = matmul(d_flat, wd_both[layer], NT)
            d_pre = gelu_pull(d_act)[0]
            d_pre_bf = d_pre.astype(BF)
            d_bup = jnp.sum(d_pre, axis=0)
            part = blocks(matmul(d_pre_bf, wu_both[layer], NT))
            d_wdown, d_wup, d_res, sum_two, da_plane = backward(
                [part, res_two, ln_par[layer, 2:3], d_res, act, d_flat, h2_flat, d_pre_bf], (True, False),
                [(n_col, width), (width, n_col)], 3, True)
            da_flat = da_plane.reshape(n_plane, width)
            d_both = matmul(da_flat, wo_both[layer], NT).astype(BF)
            dq_both, y_part = comm(attention_back_kernel, 7 + layer, [d_both, nat, stat, top_part, top_res[part_slice(layer)], bias_d[n_layers - 1, 1:2]], (
                jax.ShapeDtypeStruct((n_plane, 6 * head), BF), jax.ShapeDtypeStruct((part_rows, width), BF)), [
                pltpu.VMEM(block_shape, BF), pltpu.VMEM(nat_shape.shape[1:], BF), pltpu.VMEM((n_q, n_all), F32),
                pltpu.VMEM((n_q, n_all), F32), pltpu.VMEM((n_q, n_all), BF), pltpu.VMEM((n_q, n_all), BF),
                pltpu.VMEM((n_all, head), F32), pltpu.VMEM((n_all, head), F32), pltpu.VMEM(nat_shape.shape, BF),
                pltpu.VMEM((3,) + block_shape, BF)] + pair_sems + part_scatter, layer * part_rows)
            y_parts[layer] = y_part
            part = blocks(matmul(dq_both, wq_both[layer], NT))
            args = [part, res_one, ln_par[layer, 0:1], d_res, a_both, da_flat, h_flat, dq_both]
            shapes = [(head, width), (width, 3 * head)]
            others = [sum_two[0:2], sum_two[2:3], bias_two]
            if layer > 0:
                d_wout, d_wqkv, d_res, sum_one, d_plane = backward(args, (True, False), shapes, 4, True)
                bias_two = sum_one[2:3]
                smalls = [sum_one[0:2]] + others + smalls
            else:
                smalls = [jnp.zeros((2, width), F32)] + others + smalls
                n_small = sum(piece.shape[0] for piece in smalls)
                packed = jnp.concatenate(smalls + [jnp.zeros((-n_small % 16, width), F32)], axis=0)
                d_wout, d_wqkv, x_grad, total = backward(args + [packed], (True, False), shapes, 5, False)
            grads[layer] = (d_wqkv, d_wout, d_wup, d_bup[:n_col] + swapped(d_bup[n_col:]), d_wdown)
        total = total[:n_small].reshape(n_layers, n_small // n_layers, width)
        return (jnp.concatenate(y_parts, axis=0).reshape(x_loc.shape), x_grad.reshape(x_loc.shape), total[:, :4], total[:, 4:],
                jnp.stack([grad[0].reshape(width, 3, 1, head) for grad in grads]),
                jnp.stack([grad[1].reshape(1, head, width) for grad in grads]),
                jnp.stack([grad[2] for grad in grads]),
                jnp.stack([grad[3] for grad in grads]),
                jnp.stack([grad[4] for grad in grads]))

    def on_tp(dim, first=None):
        return P(first, *[None] * (dim - 1), 'tp')

    rows_spec = P('dp', 'tp')
    in_specs = (rows_spec, rows_spec, P(), P(), on_tp(3), on_tp(1), on_tp(2), on_tp(1), on_tp(1))
    out_specs = (rows_spec, rows_spec, P('dp'), P('dp'), on_tp(3, 'dp'), on_tp(1, 'dp'), on_tp(2, 'dp'), on_tp(1, 'dp'), on_tp(1, 'dp'))
    return jax.shard_map(device_step, mesh=mesh, in_specs=in_specs, out_specs=out_specs, check_vma=False)
```
